256 devices in a mesh: fsdp: 256 (over y, x, z, core).
Axes of the slice: x: 4, y: 4, z: 8, core: 2. Of those that a mesh axis runs over, the one named last changes fastest.
Arguments:
- tokens: bfloat16 [32768, 2048], P('fsdp'), may hold values from -6 to 6
- member_ids: int32 [256], P('fsdp'), may hold values from 0 to 3
- norm_gain: float32 [2048], replicated, may hold values from 0.1 to 6
- weight: bfloat16 [2048, 1152], P('fsdp'), may hold values from -0.125 to 0.125
- qkv_bias: float32 [1152], replicated, may hold values from -160 to 160
- fast_in: float32 [4, 2048], replicated, may hold values from 0.25 to 1.75
- fast_out: float32 [4, 1152], replicated, may hold values from 0.25 to 1.75
- cotangent: bfloat16 [32768, 896], P('fsdp'), may hold values from -64 to 64
- weight_first: float32 [2048, 1152], P('fsdp'), may hold values from -0.0007324219 to 0.0007324219
- weight_second: float32 [2048, 1152], P('fsdp'), may hold values from 1e-09 to 1e-07
- in_first: float32 [4, 2048], replicated, may hold values from -0.015625 to 0.015625
- in_second: float32 [4, 2048], replicated, may hold values from 1e-07 to 1e-05
- out_first: float32 [4, 1152], replicated, may hold values from -0.015625 to 0.015625
- out_second: float32 [4, 1152], replicated, may hold values from 1e-07 to 1e-05
Outputs:
- weight_step: float32 [2048, 1152], P('fsdp')
- in_step: float32 [4, 2048], replicated
- out_step: float32 [4, 1152], replicated
The draws below stay inside these ranges and needn't reach their ends.
All inputs are finite; a program needn't handle non-finite values.
Results may differ from the reference program's by a relative error of at most 0.0045.
The reference program's roundings to bfloat16 on the way (of `scaled`, `grad_scores` and `grad_down`) count: a program that leaves them out, or rounds other values in their place, can miss the bound.
Values may be sent and summed in bfloat16 or wider, within the bound.
No kernel may reach another device: no remote copies, remote signals or barrier semaphores. Data moves between devices by JAX's collectives and lax.ppermute only.
A program may use at most 128 MiB of HBM per device.

```python
import math
import jax
import jax.numpy as jnp
from jax import lax

D = 2048
HEADS = 14
KV_HEADS = 2
HEAD_DIM = 64
MEMBERS = 4
SEQS = 256
TOKENS = 32768
QW = 896
QKV = 1152
N_FSDP = 256


def draw_norm_gain(key, part):
    placing = jnp.arange(D, dtype=jnp.float32) / D
    rough = jax.random.uniform(jax.random.fold_in(key, 11), (D,), jnp.float32, -0.4, 0.4)
    return 0.5 * jnp.exp(0.5 * math.log(10.0) * placing + rough)


def draw_qkv_bias(key, part):
    drawn = 0.5 * jnp.clip(jax.random.normal(jax.random.fold_in(key, 21), (QKV,), jnp.float32), -6.0, 6.0)
    return drawn


def draw_cotangent(key, part):
    row_key = jax.random.fold_in(key, 31)
    col_key = jax.random.fold_in(key, 32)
    noise_key = jax.random.fold_in(key, 33)
    row_scale = jnp.exp(jax.random.uniform(row_key, (TOKENS, 1), jnp.float32, math.log(0.3), math.log(3.0)))
    col_scale = jnp.exp(jax.random.uniform(col_key, (1, QW), jnp.float32, math.log(0.3), math.log(3.0)))
    noise = jnp.clip(jax.random.normal(noise_key, (TOKENS, QW), jnp.float32), -6.0, 6.0)
    return (row_scale * col_scale * noise).astype(jnp.bfloat16)


def touch_ends(values, rng, smallest, high):
    longest = values.shape.index(max(values.shape))
    spots = []
    for shift in (0, 1):
        where = [jax.random.randint(jax.random.fold_in(rng, axis), (), 0, length) for axis, length in enumerate(values.shape)]
        where[longest] = (where[longest] + shift) % values.shape[longest]
        spots.append(tuple(where))
    return values.at[spots[0]].set(smallest).at[spots[1]].set(high)


def levels(own_key, shape, split, least, high):
    level = 1.0
    for axis_at, blocks in split:
        heights = jax.random.uniform(jax.random.fold_in(jax.random.fold_in(own_key, 6), axis_at), (blocks,), jnp.float32, least / len(split), high / len(split))
        level = level * jnp.repeat(jnp.exp(heights), shape[axis_at] // blocks).reshape((-1,) + (1,) * (len(shape) - 1 - axis_at))
    return level


def gaussian(own_key, dims, scale, most, shards=(), held_as=jnp.bfloat16):
    array = jax.random.normal(own_key, dims, jnp.float32) * scale
    if len(shards) > 0:
        array = levels(own_key, dims, shards, -0.22, 0.18) * array
    return jnp.clip(array, min=-most, max=most).astype(held_as)


def setup_inputs(seed: int = 0) -> dict:
    streams_of = jax.random.split(jax.random.key(seed), 15)
    return {
        "tokens": gaussian(streams_of[0], (TOKENS, D), 1.0, 6.0, ((0, 256),)),
        "member_ids": touch_ends(jax.random.randint(streams_of[1], (SEQS,), 0, MEMBERS), jax.random.fold_in(streams_of[1], 1), 0, MEMBERS - 1).astype(jnp.int32),
        "norm_gain": draw_norm_gain(jax.random.fold_in(streams_of[14], 71), 0),
        "weight": gaussian(streams_of[3], (D, QKV), D ** -0.5, 0.125, ((0, 256),)),
        "qkv_bias": draw_qkv_bias(jax.random.fold_in(streams_of[14], 71), 0),
        "fast_in": jnp.clip(1.0 + 0.15 * jax.random.normal(streams_of[5], (MEMBERS, D), jnp.float32), 0.25, 1.75),
        "fast_out": jnp.clip(1.0 + 0.15 * jax.random.normal(streams_of[6], (MEMBERS, QKV), jnp.float32), 0.25, 1.75),
        "cotangent": draw_cotangent(jax.random.fold_in(streams_of[14], 71), 0),
        "weight_first": gaussian(streams_of[8], (D, QKV), 0.00005, 0.0007324219, ((0, 256),), jnp.float32),
        "weight_second": jnp.clip(jnp.exp(math.log(1.0000000116860974e-07) - 4.6051702 * jax.random.uniform(streams_of[9], (D, QKV), jnp.float32) ** levels(streams_of[9], (D, QKV), ((0, 256),), -0.2, 0.2)), 9.999999717180685e-10, 1.0000000116860974e-07),
        "in_first": gaussian(streams_of[10], (MEMBERS, D), 0.001, 0.015625, (), jnp.float32),
        "in_second": jnp.clip(jnp.exp(jax.random.uniform(streams_of[11], (MEMBERS, D), jnp.float32, math.log(1.0000000116860974e-07), math.log(9.999999747378752e-06))), 1.0000000116860974e-07, 9.999999747378752e-06),
        "out_first": gaussian(streams_of[12], (MEMBERS, QKV), 0.001, 0.015625, (), jnp.float32),
        "out_second": jnp.clip(jnp.exp(jax.random.uniform(streams_of[13], (MEMBERS, QKV), jnp.float32, math.log(1.0000000116860974e-07), math.log(9.999999747378752e-06))), 1.0000000116860974e-07, 9.999999747378752e-06),
    }


norm_eps = 1e-06
clip_limit = 1.0
beta_one = 0.9
beta_two = 0.95
adam_eps = 1e-08
rope_base = 1000000.0
step_number = 10.0

def rope_tables(seq_length, head_width):
    half_width = head_width // 2
    spacing = jnp.arange(half_width, dtype=jnp.float32) * (2.0 / head_width)
    frequency = jnp.exp(-math.log(rope_base) * spacing)
    angles = jnp.arange(seq_length, dtype=jnp.float32)[:, None] * frequency[None, :]
    return (jnp.cos(angles), jnp.sin(angles))

def rotate(features, cosine_table, sine_table):
    half_width = features.shape[-1] // 2
    first_half = features[..., :half_width]
    second_half = features[..., half_width:]
    cosine_rows = cosine_table[:, None, :]
    sine_rows = sine_table[:, None, :]
    return jnp.concatenate([first_half * cosine_rows - second_half * sine_rows, second_half * cosine_rows + first_half * sine_rows], axis=-1)

def member_sum(onehot, values):
    return lax.dot_general(onehot, values, (((0,), (0,)), ((), ())), precision=lax.Precision.HIGHEST)

def block_grads(tokens, member_ids, norm_gain, gathered, qkv_bias, fast_in, fast_out, cotangent, head_count, kv_count, head_width):
    members = fast_in.shape[0]
    seq_count = member_ids.shape[0]
    tok_count = tokens.shape[0]
    seq_length = tok_count // seq_count
    group_size = head_count // kv_count
    q_width = head_count * head_width
    kv_width = kv_count * head_width
    token_member = jnp.repeat(member_ids, seq_length, total_repeat_length=tok_count)
    onehot = (token_member[:, None] == jnp.arange(members, dtype=jnp.int32)[None, :]).astype(jnp.float32)
    highest = lax.Precision.HIGHEST
    scale_in = jnp.dot(onehot, fast_in, precision=highest)
    scale_out = jnp.dot(onehot, fast_out, precision=highest)
    widened = tokens.astype(jnp.float32)
    normed = widened * lax.rsqrt(lax.optimization_barrier(jnp.mean(widened * widened, axis=1, keepdims=True)) + norm_eps) * norm_gain[None, :]
    scaled = (normed * scale_in).astype(jnp.bfloat16)
    projected = jnp.dot(scaled, gathered, preferred_element_type=jnp.float32)
    biased = projected * scale_out + qkv_bias[None, :]
    cosine_table, sine_table = rope_tables(seq_length, head_width)
    queries = rotate(biased[:, :q_width].reshape(seq_count, seq_length, head_count, head_width), cosine_table, sine_table).astype(jnp.bfloat16)
    key_heads = rotate(biased[:, q_width:q_width + kv_width].reshape(seq_count, seq_length, kv_count, head_width), cosine_table, sine_table).astype(jnp.bfloat16)
    value_heads = biased[:, q_width + kv_width:].reshape(seq_count, seq_length, kv_count, head_width).astype(jnp.bfloat16)
    queries = queries.reshape(seq_count, seq_length, kv_count, group_size, head_width)
    upstream = cotangent.reshape(seq_count, seq_length, kv_count, group_size, head_width)
    score_scale = 1.0 / math.sqrt(head_width)
    scores = jnp.einsum('sqgrd,skgd->sgrqk', queries.astype(jnp.float32), key_heads.astype(jnp.float32)) * score_scale
    causal = jnp.arange(seq_length)[:, None] >= jnp.arange(seq_length)[None, :]
    scores = jnp.where(causal, scores, -jnp.inf)
    probabilities = jnp.exp(scores - lax.optimization_barrier(jnp.max(scores, axis=-1, keepdims=True)))
    probabilities = probabilities / lax.optimization_barrier(jnp.sum(probabilities, axis=-1, keepdims=True))
    rounded = probabilities.astype(jnp.bfloat16)
    grad_value = jnp.einsum('sgrqk,sqgrd->skgd', rounded.astype(jnp.float32), upstream.astype(jnp.float32))
    grad_probs = jnp.einsum('sqgrd,skgd->sgrqk', upstream.astype(jnp.float32), value_heads.astype(jnp.float32))
    grad_scores = (probabilities * (grad_probs - lax.optimization_barrier(jnp.sum(grad_probs * probabilities, axis=-1, keepdims=True))) * score_scale).astype(jnp.bfloat16)
    grad_query = jnp.einsum('sgrqk,skgd->sqgrd', grad_scores.astype(jnp.float32), key_heads.astype(jnp.float32))
    grad_key = jnp.einsum('sgrqk,sqgrd->skgd', grad_scores.astype(jnp.float32), queries.astype(jnp.float32))
    grad_query = rotate(grad_query.reshape(seq_count, seq_length, head_count, head_width), cosine_table, -sine_table).reshape(tok_count, q_width)
    grad_key = rotate(grad_key, cosine_table, -sine_table).reshape(tok_count, kv_width)
    grad_biased = jnp.concatenate([grad_query, grad_key, grad_value.reshape(tok_count, kv_width)], axis=1)
    out_part = member_sum(onehot, projected * grad_biased)
    grad_down = (grad_biased * scale_out).astype(jnp.bfloat16)
    weight_part = lax.dot_general(scaled, grad_down, (((0,), (0,)), ((), ())), preferred_element_type=jnp.float32)
    back = lax.dot_general(grad_down, gathered, (((1,), (1,)), ((), ())), preferred_element_type=jnp.float32)
    in_part = member_sum(onehot, normed * back)
    return (weight_part, in_part, out_part)

def adam_direction(gradient, moment_one, moment_two, clip_scale):
    clipped = gradient * clip_scale
    first_new = beta_one * moment_one + (1.0 - beta_one) * clipped
    second_new = beta_two * moment_two + (1.0 - beta_two) * clipped * clipped
    first_hat = first_new / (1.0 - beta_one ** step_number)
    second_hat = second_new / (1.0 - beta_two ** step_number)
    return first_hat / (jnp.sqrt(second_hat) + adam_eps)

def reference(tokens, member_ids, norm_gain, weight, qkv_bias, fast_in, fast_out, cotangent, weight_first, weight_second, in_first, in_second, out_first, out_second):
    blocks = N_FSDP
    tok_blocks = tokens.reshape(blocks, -1, tokens.shape[1])
    id_blocks = member_ids.reshape(blocks, -1)
    cot_blocks = cotangent.reshape(blocks, -1, cotangent.shape[1])

    def accumulate(carry, pieces):
        parts = block_grads(pieces[0], pieces[1], norm_gain, weight, qkv_bias, fast_in, fast_out, pieces[2], HEADS, KV_HEADS, HEAD_DIM)
        return ((carry[0] + parts[0], carry[1] + parts[1], carry[2] + parts[2]), None)
    start_carry = (jnp.zeros(weight.shape, jnp.float32), jnp.zeros(fast_in.shape, jnp.float32), jnp.zeros(fast_out.shape, jnp.float32))
    totals, _ = lax.scan(accumulate, start_carry, (tok_blocks, id_blocks, cot_blocks))
    weight_grad, in_grad, out_grad = totals
    squared = jnp.sum(weight_grad * weight_grad) + jnp.sum(in_grad * in_grad) + jnp.sum(out_grad * out_grad)
    grad_norm = jnp.sqrt(squared)
    clip_scale = clip_limit / jnp.maximum(grad_norm, clip_limit)
    weight_step = adam_direction(weight_grad, weight_first, weight_second, clip_scale)
    in_step = adam_direction(in_grad, in_first, in_second, clip_scale)
    out_step = adam_direction(out_grad, out_first, out_second, clip_scale)
    return (weight_step, in_step, out_step)
```

```python
import functools
import math

import jax
import jax.numpy as jnp
from jax import lax
from jax.experimental import pallas as pl
from jax.experimental.pallas import tpu as pltpu
from jax.sharding import PartitionSpec as P

AXIS = "fsdp"
NY, NX, NZ = 4, 4, 8
HEADS = 14
KV_HEADS = 2
HEAD_DIM = 64
GROUP_Q = 448
GROUP_W = 576
LANES = 640
SEQ = 128
FEATURES = 2048
TILES = FEATURES // 128

norm_eps = 1e-06
clip_limit = 1.0
beta_one = 0.9
beta_two = 0.95
adam_eps = 1e-08
rope_base = 1000000.0
step_number = 10.0


f32 = jnp.float32
bf16 = jnp.bfloat16


def device_of(y, x, z, c):
    return ((y * NX + x) * NZ + z) * 2 + c


Z_RINGS = [
    [device_of(y, x, z, c) for z in range(NZ)] for y in range(NY) for x in range(NX) for c in range(2)
]
PAIRS = [
    [device_of(y, x, z, c) for c in range(2)] for y in range(NY) for x in range(NX) for z in range(NZ)
]
INNER_RINGS = [
    [device_of(y, x, z, 0) for x in range(NX)] for y in range(NY) for z in range(NZ)
] + [[device_of(y, x, z, 1) for y in range(NY)] for x in range(NX) for z in range(NZ)]
OUTER_RINGS = [
    [device_of(y, x, z, 0) for y in range(NY)] for x in range(NX) for z in range(NZ)
] + [[device_of(y, x, z, 1) for x in range(NX)] for y in range(NY) for z in range(NZ)]


def shift(array, rings, step):
    pairs = [(ring[i], ring[(i + step) % len(ring)]) for ring in rings for i in range(len(ring))]
    return lax.ppermute(array, AXIS, pairs)


def rope_tables():
    half_width = HEAD_DIM // 2
    spacing = jnp.arange(half_width, dtype=f32) * (2.0 / HEAD_DIM)
    frequency = jnp.exp(-math.log(rope_base) * spacing)
    angles = jnp.arange(SEQ, dtype=f32)[:, None] * frequency[None, :]
    cosine, sine = jnp.cos(angles), jnp.sin(angles)
    return (
        jnp.concatenate([cosine] * 4, axis=1),
        jnp.concatenate([-sine, sine, -sine, sine], axis=1),
    )


def dot(left, right, left_dim, right_dim):
    return lax.dot_general(
        left, right, (((left_dim,), (right_dim,)), ((), ())), preferred_element_type=f32
    )


def scale_kernel(tile_of, own, partner, gain, rates, scaled, inverse):
    for part, tokens in enumerate((own, partner)):
        rows = slice(part * SEQ, (part + 1) * SEQ)
        wide = tokens[...].astype(f32)
        inv = lax.rsqrt(jnp.mean(wide * wide, axis=1, keepdims=True) + norm_eps)
        inverse[rows, :] = jnp.broadcast_to(inv, (SEQ, 128))
        for i in range(TILES):
            lanes = pl.ds(pl.multiple_of(tile_of[i] * 128, 128), 128)
            normed = tokens[:, lanes].astype(f32) * inv * gain[:, lanes]
            scaled[rows, i * 128 : (i + 1) * 128] = (normed * rates[part : part + 1, lanes]).astype(bf16)


def attention_kernel(
    members, scaled, w0, w1, w2, w3, slopes, bias, cosine_ref, sine_ref, cot_own, cot_partner, down, out_cols
):
    cosine = cosine_ref[...]
    sine = sine_ref[...]
    lane = lax.broadcasted_iota(jnp.int32, (SEQ, 128), 1)
    row = lax.broadcasted_iota(jnp.int32, (SEQ, 128), 0)
    low = lane < 64
    first = (lane & 63) < 32
    causal = row >= lane
    score_scale = 1.0 / math.sqrt(HEAD_DIM)

    def swap(tile):
        return jnp.where(first, pltpu.roll(tile, 96, 1), pltpu.roll(tile, 32, 1))

    def half_turn(tile):
        return pltpu.roll(tile, 64, 1)

    projected = sum(
        dot(scaled[:, j * 512 : (j + 1) * 512], w[...], 1, 0) for j, w in enumerate((w0, w1, w2, w3))
    )
    totals = []
    for part, cot in enumerate((cot_own, cot_partner)):
        rows = slice(part * SEQ, (part + 1) * SEQ)
        raw = projected[rows]
        slope = slopes[part : part + 1, :]
        biased = raw * slope + bias[...]
        turned = []
        for t in range(4):
            tile = biased[:, t * 128 : (t + 1) * 128]
            turned.append(tile * cosine + swap(tile) * sine)
        keys = turned[3]
        values = biased[:, 512:640]
        key_pair = jnp.concatenate(
            [jnp.where(low, half_turn(keys), 0.0), jnp.where(low, 0.0, keys)], axis=0
        ).astype(bf16)
        value_pair = jnp.concatenate(
            [jnp.where(low, values, 0.0), jnp.where(low, 0.0, half_turn(values))], axis=0
        ).astype(bf16)
        grads = []
        key_sum = jnp.zeros((2 * SEQ, 128), f32)
        value_sum = jnp.zeros((2 * SEQ, 128), f32)
        for t in range(4):
            query = turned[t].astype(bf16)
            upstream = cot[:, t * 128 : (t + 1) * 128]
            scores = dot(query, key_pair, 1, 1) * score_scale
            grad_probs = dot(upstream, value_pair, 1, 1)
            probs_bf, grads_bf = [], []
            for h in range(2):
                side = slice(h * SEQ, (h + 1) * SEQ)
                masked = jnp.where(causal, scores[:, side], -jnp.inf)
                raised = jnp.exp(masked - jnp.max(masked, axis=1, keepdims=True))
                probs = raised / jnp.sum(raised, axis=1, keepdims=True)
                gp = grad_probs[:, side]
                centre = jnp.sum(gp * probs, axis=1, keepdims=True)
                probs_bf.append(probs.astype(bf16))
                grads_bf.append((probs * (gp - centre) * score_scale).astype(bf16))
            probs_pair = jnp.concatenate(probs_bf, axis=1)
            grad_pair = jnp.concatenate(grads_bf, axis=1)
            grads.append(dot(grad_pair, key_pair, 1, 0))
            key_sum += dot(grad_pair, query, 0, 0)
            value_sum += dot(probs_pair, upstream, 0, 0)
        grad_key = jnp.where(low, 0.0, half_turn(key_sum[:SEQ]) + key_sum[SEQ:])
        grad_value = jnp.where(low, value_sum[:SEQ] + half_turn(value_sum[SEQ:]), 0.0)
        grads[3] = jnp.where(low, grads[3], grad_key)
        grads = [g * cosine - swap(g) * sine for g in grads] + [grad_value]
        grad_biased = jnp.concatenate(grads, axis=1)
        totals.append(jnp.sum(raw * grad_biased, axis=0, keepdims=True))
        down[rows, :] = (grad_biased * slope).astype(bf16)
    for t in range(5):
        lanes = slice(t * 128, (t + 1) * 128)
        spread = jnp.where(row == 68 + members[0], totals[0][:, lanes], 0.0)
        spread += jnp.where(row == 68 + members[1], totals[1][:, lanes], 0.0)
        out_cols[lanes, :] = spread.T


def weight_kernel(block, tile_of, members, own, partner, gain, inverse, scaled, down, w, out_cols, result):
    row = lax.broadcasted_iota(jnp.int32, (128, 128), 0)
    grad_down = down[...]
    part_grad = dot(scaled[:, block * 512 : (block + 1) * 512], grad_down, 0, 0)
    back = dot(grad_down, w[...], 1, 1)
    for i in range(4):
        tile = tile_of[block * 4 + i]
        lanes = pl.ds(pl.multiple_of(tile * 128, 128), 128)
        spread = jnp.zeros((128, 128), f32)
        for part, tokens in enumerate((own, partner)):
            rows = slice(part * SEQ, (part + 1) * SEQ)
            normed = tokens[:, lanes].astype(f32) * inverse[rows, :] * gain[:, lanes]
            total = jnp.sum(normed * back[rows, i * 128 : (i + 1) * 128], axis=0, keepdims=True)
            spread += jnp.where(row == 64 + members[part], total, 0.0)
        extra = spread.T
        spot = pl.multiple_of(jnp.minimum(tile, 4) * 128, 128)
        extra += jnp.where(tile < 5, out_cols[pl.ds(spot, 128), :], 0.0)
        here = slice(i * 128, (i + 1) * 128)
        result[here, :512] = part_grad[here, :512].astype(result.dtype)
        result[here, 512:] = (part_grad[here, 512:] + extra).astype(result.dtype)


SMEM = pl.BlockSpec(memory_space=pltpu.SMEM)
VMEM = pl.BlockSpec(memory_space=pltpu.VMEM)


def call(kernel, scalars, arrays, out_shape, name):
    single = not isinstance(out_shape, (list, tuple))
    return pl.pallas_call(
        kernel,
        in_specs=[SMEM] * len(scalars) + [VMEM] * len(arrays),
        out_specs=VMEM if single else [VMEM] * len(out_shape),
        out_shape=out_shape,
        name=name,
        compiler_params=pltpu.CompilerParams(vmem_limit_bytes=48 * 1024 * 1024),
    )(*scalars, *arrays)


def group_columns(array, group):
    pieces = [
        array[:, group * GROUP_Q : (group + 1) * GROUP_Q],
        array[:, 896 + group * 64 : 960 + group * 64],
        array[:, 1024 + group * 64 : 1088 + group * 64],
    ]
    return jnp.concatenate(pieces, axis=1)


def whole_columns(zero, one):
    return jnp.concatenate(
        [
            zero[:, :448],
            one[:, :448],
            zero[:, 448:512],
            one[:, 448:512],
            zero[:, 512:576],
            one[:, 512:576],
        ],
        axis=1,
    )


def pad_lanes(array, width):
    return jnp.pad(array, ((0, 0), (0, width - array.shape[1])))


def adam_direction(gradient, moment_one, moment_two, clip_scale):
    clipped = gradient * clip_scale
    first_new = beta_one * moment_one + (1.0 - beta_one) * clipped
    second_new = beta_two * moment_two + (1.0 - beta_two) * clipped * clipped
    first_hat = first_new / (1.0 - beta_one**step_number)
    second_hat = second_new / (1.0 - beta_two**step_number)
    return first_hat / (jnp.sqrt(second_hat) + adam_eps)


def per_device(
    tokens,
    member_ids,
    norm_gain,
    weight,
    qkv_bias,
    fast_in,
    fast_out,
    cotangent,
    weight_first,
    weight_second,
    in_first,
    in_second,
    out_first,
    out_second,
):
    here = lax.axis_index(AXIS)
    core = here % 2
    z_spot = (here // 2) % NZ
    del z_spot
    x_spot = (here // (2 * NZ)) % NX
    y_spot = here // (2 * NZ * NX)
    is_zero = core == 0

    zero_cols = pad_lanes(group_columns(weight, 0), LANES)
    one_cols = pad_lanes(group_columns(weight, 1), LANES)
    mine = jnp.where(is_zero, zero_cols, one_cols)
    given = shift(jnp.where(is_zero, one_cols, zero_cols), PAIRS, 1)
    chip_rows = jnp.where(is_zero, jnp.concatenate([mine, given]), jnp.concatenate([given, mine]))

    partner_tokens = shift(tokens, PAIRS, 1)
    cot_zero = pad_lanes(cotangent[:, :GROUP_Q], 512)
    cot_one = pad_lanes(cotangent[:, GROUP_Q:], 512)
    cot_own = jnp.where(is_zero, cot_zero, cot_one)
    cot_partner = shift(jnp.where(is_zero, cot_one, cot_zero), PAIRS, 1)
    member_tile = jnp.broadcast_to(member_ids.astype(f32)[:, None], (8, 128))
    partner_member = shift(member_tile, PAIRS, 1)[0, 0].astype(jnp.int32)
    members = jnp.stack([member_ids[0], partner_member])
    pick = (members[:, None] == jnp.arange(4, dtype=jnp.int32)[None, :]).astype(f32)
    rates = jnp.sum(pick[:, :, None] * fast_in[None], axis=1)
    slopes_all = jnp.sum(pick[:, :, None] * fast_out[None], axis=1)
    slopes = pad_lanes(
        jnp.where(is_zero, group_columns(slopes_all, 0), group_columns(slopes_all, 1)), LANES
    )
    bias_all = qkv_bias[None, :]
    bias = pad_lanes(jnp.where(is_zero, group_columns(bias_all, 0), group_columns(bias_all, 1)), LANES)
    gain = norm_gain[None, :]
    cosine, sine = rope_tables()

    turn = jnp.arange(TILES, dtype=jnp.int32)
    outer, inner = turn // 4, turn % 4
    y_back = jnp.where(is_zero, outer, inner)
    x_back = jnp.where(is_zero, inner, outer)
    tile_of = ((y_spot - y_back) % NY) * NX + (x_spot - x_back) % NX

    spread = jnp.broadcast_to(chip_rows[None], (NZ, 16, LANES))
    column = lax.all_to_all(
        spread, AXIS, split_axis=0, concat_axis=0, tiled=True, axis_index_groups=Z_RINGS
    ).reshape(NZ * 16, LANES)
    plane = jnp.concatenate([column] + [shift(column, INNER_RINGS, j) for j in (1, 2, 3)], axis=0)
    rows_of = [plane] + [shift(plane, OUTER_RINGS, j) for j in (1, 2, 3)]

    scaled, inverse = call(
        scale_kernel,
        [tile_of],
        [tokens, partner_tokens, gain, rates],
        [
            jax.ShapeDtypeStruct((2 * SEQ, FEATURES), bf16),
            jax.ShapeDtypeStruct((2 * SEQ, 128), f32),
        ],
        "scale",
    )
    down, out_cols = call(
        attention_kernel,
        [members],
        [scaled, *rows_of, slopes, bias, cosine, sine, cot_own, cot_partner],
        [
            jax.ShapeDtypeStruct((2 * SEQ, LANES), bf16),
            jax.ShapeDtypeStruct((LANES, 128), f32),
        ],
        "attention",
    )

    def block_grad(block):
        return call(
            functools.partial(weight_kernel, block),
            [tile_of, members],
            [tokens, partner_tokens, gain, inverse, scaled, down, rows_of[block], out_cols],
            jax.ShapeDtypeStruct((512, LANES), f32 if block == 0 else bf16),
            "weight_grad",
        )

    got = [shift(block_grad(j), OUTER_RINGS, -j) for j in (2, 1, 3)]
    plane_sum = block_grad(0) + sum(g.astype(f32) for g in got)
    parts = [plane_sum[j * 128 : (j + 1) * 128] for j in range(4)]
    got = [shift(parts[j].astype(bf16), INNER_RINGS, -j) for j in (2, 1, 3)]
    column_sum = parts[0] + sum(g.astype(f32) for g in got)
    pieces = lax.all_to_all(
        column_sum.astype(bf16).reshape(NZ, 16, LANES),
        AXIS,
        split_axis=0,
        concat_axis=0,
        tiled=True,
        axis_index_groups=Z_RINGS,
    )
    chip_sum = jnp.sum(pieces.astype(f32), axis=0)
    keep = jnp.where(is_zero, chip_sum[:8], chip_sum[8:])
    given = shift(jnp.where(is_zero, chip_sum[8:], chip_sum[:8]), PAIRS, 1)
    from_zero = jnp.where(is_zero, keep, given)
    from_one = jnp.where(is_zero, given, keep)
    grad_rows = whole_columns(from_zero, from_one)

    own_in = from_zero[:, 576:580] + from_one[:, 576:580]
    shares = jnp.concatenate([own_in, from_zero[:, 580:584], from_one[:, 580:584]], axis=1)
    square = jnp.sum(grad_rows * grad_rows).reshape(1, 1)
    packed = pad_lanes(jnp.concatenate([shares.reshape(1, 96), square], axis=1), 128)
    everyone = lax.all_to_all(
        jnp.broadcast_to(packed[:, None], (256, 1, 128)), AXIS, split_axis=0, concat_axis=0, tiled=True
    ).reshape(256, 128)
    weight_square = jnp.sum(everyone[:, 96])
    share_all = everyone[:, :96].reshape(256, 8, 12)
    in_grad = share_all[:, :, 0:4].reshape(FEATURES, 4).T
    out_zero = share_all[:72, :, 4:8].reshape(GROUP_W, 4).T
    out_one = share_all[:72, :, 8:12].reshape(GROUP_W, 4).T
    out_grad = whole_columns(out_zero, out_one)

    squared = weight_square + jnp.sum(in_grad * in_grad) + jnp.sum(out_grad * out_grad)
    clip_scale = clip_limit / jnp.maximum(jnp.sqrt(squared), clip_limit)
    weight_step = adam_direction(grad_rows, weight_first, weight_second, clip_scale)
    in_step = adam_direction(in_grad, in_first, in_second, clip_scale)
    out_step = adam_direction(out_grad, out_first, out_second, clip_scale)
    return (weight_step, in_step, out_step)


def solution(mesh):
    return jax.shard_map(
        per_device,
        mesh=mesh,
        in_specs=(
            P(AXIS, None),
            P(AXIS),
            P(),
            P(AXIS, None),
            P(),
            P(),
            P(),
            P(AXIS, None),
            P(AXIS, None),
            P(AXIS, None),
            P(),
            P(),
            P(),
            P(),
        ),
        out_specs=(P(AXIS, None), P(), P()),
        check_vma=False,
    )
```

```python
import functools
import math

import jax
import jax.numpy as jnp
from jax import lax
from jax.experimental import pallas as pl
from jax.experimental.pallas import tpu as pltpu
from jax.sharding import PartitionSpec as P

AXIS = "fsdp"
NY, NX, NZ = 4, 4, 8
HEADS = 14
KV_HEADS = 2
HEAD_DIM = 64
GROUP_Q = 448
GROUP_W = 576
LANES = 640
SEQ = 128
FEATURES = 2048
TILES = FEATURES // 128

norm_eps = 1e-06
clip_limit = 1.0
beta_one = 0.9
beta_two = 0.95
adam_eps = 1e-08
rope_base = 1000000.0
step_number = 10.0


f32 = jnp.float32
bf16 = jnp.bfloat16


def device_of(y, x, z, c):
    return ((y * NX + x) * NZ + z) * 2 + c


COLUMNS = [
    [device_of(y, x, z, c) for z in range(NZ) for c in range(2)] for y in range(NY) for x in range(NX)
]
PAIRS = [
    [device_of(y, x, z, c) for c in range(2)] for y in range(NY) for x in range(NX) for z in range(NZ)
]
INNER_RINGS = [
    [device_of(y, x, z, 0) for x in range(NX)] for y in range(NY) for z in range(NZ)
] + [[device_of(y, x, z, 1) for y in range(NY)] for x in range(NX) for z in range(NZ)]
OUTER_RINGS = [
    [device_of(y, x, z, 0) for y in range(NY)] for x in range(NX) for z in range(NZ)
] + [[device_of(y, x, z, 1) for x in range(NX)] for y in range(NY) for z in range(NZ)]


def shift(array, rings, step):
    pairs = [(ring[i], ring[(i + step) % len(ring)]) for ring in rings for i in range(len(ring))]
    return lax.ppermute(array, AXIS, pairs)


def rope_tables():
    half_width = HEAD_DIM // 2
    spacing = jnp.arange(half_width, dtype=f32) * (2.0 / HEAD_DIM)
    frequency = jnp.exp(-math.log(rope_base) * spacing)
    angles = jnp.arange(SEQ, dtype=f32)[:, None] * frequency[None, :]
    cosine, sine = jnp.cos(angles), jnp.sin(angles)
    return (
        jnp.concatenate([cosine] * 4, axis=1),
        jnp.concatenate([-sine, sine, -sine, sine], axis=1),
    )


def dot(left, right, left_dim, right_dim):
    return lax.dot_general(
        left, right, (((left_dim,), (right_dim,)), ((), ())), preferred_element_type=f32
    )


def scale_kernel(tile_of, own, partner, gain, rates, scaled, inverse):
    for part, tokens in enumerate((own, partner)):
        rows = slice(part * SEQ, (part + 1) * SEQ)
        wide = tokens[...].astype(f32)
        inv = lax.rsqrt(jnp.mean(wide * wide, axis=1, keepdims=True) + norm_eps)
        inverse[rows, :] = jnp.broadcast_to(inv, (SEQ, 128))
        for i in range(TILES):
            lanes = pl.ds(pl.multiple_of(tile_of[i] * 128, 128), 128)
            normed = tokens[:, lanes].astype(f32) * inv * gain[:, lanes]
            scaled[rows, i * 128 : (i + 1) * 128] = (normed * rates[part : part + 1, lanes]).astype(bf16)


def attention_kernel(members, *refs):
    scaled, halves = refs[0], refs[1:9]
    slopes, bias, cosine_ref, sine_ref, cot_own, cot_partner, down, out_cols = refs[9:]
    cosine = cosine_ref[...]
    sine = sine_ref[...]
    lane = lax.broadcasted_iota(jnp.int32, (SEQ, 128), 1)
    row = lax.broadcasted_iota(jnp.int32, (SEQ, 128), 0)
    low = lane < 64
    first = (lane & 63) < 32
    causal = row >= lane
    score_scale = 1.0 / math.sqrt(HEAD_DIM)

    def swap(tile):
        return jnp.where(first, pltpu.roll(tile, 96, 1), pltpu.roll(tile, 32, 1))

    def half_turn(tile):
        return pltpu.roll(tile, 64, 1)

    projected = sum(
        dot(scaled[:, j * 256 : (j + 1) * 256], w[...], 1, 0) for j, w in enumerate(halves)
    )
    totals = []
    for part, cot in enumerate((cot_own, cot_partner)):
        rows = slice(part * SEQ, (part + 1) * SEQ)
        raw = projected[rows]
        slope = slopes[part : part + 1, :]
        biased = raw * slope + bias[...]
        turned = []
        for t in range(4):
            tile = biased[:, t * 128 : (t + 1) * 128]
            turned.append(tile * cosine + swap(tile) * sine)
        keys = turned[3]
        values = biased[:, 512:640]
        key_pair = jnp.concatenate(
            [jnp.where(low, half_turn(keys), 0.0), jnp.where(low, 0.0, keys)], axis=0
        ).astype(bf16)
        value_pair = jnp.concatenate(
            [jnp.where(low, values, 0.0), jnp.where(low, 0.0, half_turn(values))], axis=0
        ).astype(bf16)
        grads = []
        key_sum = jnp.zeros((2 * SEQ, 128), f32)
        value_sum = jnp.zeros((2 * SEQ, 128), f32)
        for t in range(4):
            query = turned[t].astype(bf16)
            upstream = cot[:, t * 128 : (t + 1) * 128]
            scores = dot(query, key_pair, 1, 1) * score_scale
            grad_probs = dot(upstream, value_pair, 1, 1)
            probs_bf, grads_bf = [], []
            for h in range(2):
                side = slice(h * SEQ, (h + 1) * SEQ)
                masked = jnp.where(causal, scores[:, side], -jnp.inf)
                raised = jnp.exp(masked - jnp.max(masked, axis=1, keepdims=True))
                probs = raised / jnp.sum(raised, axis=1, keepdims=True)
                gp = grad_probs[:, side]
                centre = jnp.sum(gp * probs, axis=1, keepdims=True)
                probs_bf.append(probs.astype(bf16))
                grads_bf.append((probs * (gp - centre) * score_scale).astype(bf16))
            probs_pair = jnp.concatenate(probs_bf, axis=1)
            grad_pair = jnp.concatenate(grads_bf, axis=1)
            grads.append(dot(grad_pair, key_pair, 1, 0))
            key_sum += dot(grad_pair, query, 0, 0)
            value_sum += dot(probs_pair, upstream, 0, 0)
        grad_key = jnp.where(low, 0.0, half_turn(key_sum[:SEQ]) + key_sum[SEQ:])
        grad_value = jnp.where(low, value_sum[:SEQ] + half_turn(value_sum[SEQ:]), 0.0)
        grads[3] = jnp.where(low, grads[3], grad_key)
        grads = [g * cosine - swap(g) * sine for g in grads] + [grad_value]
        grad_biased = jnp.concatenate(grads, axis=1)
        totals.append(jnp.sum(raw * grad_biased, axis=0, keepdims=True))
        down[rows, :] = (grad_biased * slope).astype(bf16)
    for t in range(5):
        lanes = slice(t * 128, (t + 1) * 128)
        spread = jnp.where(row == 68 + members[0], totals[0][:, lanes], 0.0)
        spread += jnp.where(row == 68 + members[1], totals[1][:, lanes], 0.0)
        out_cols[lanes, :] = spread.T


def weight_kernel(
    block, tile_of, members, own, partner, gain, inverse, scaled, down, wa, wb, out_cols, result_a, result_b
):
    row = lax.broadcasted_iota(jnp.int32, (128, 128), 0)
    grad_down = down[...]
    for half, (w, result) in enumerate(((wa, result_a), (wb, result_b))):
        base = block * 512 + half * 256
        part_grad = dot(scaled[:, base : base + 256], grad_down, 0, 0)
        back = dot(grad_down, w[...], 1, 1)
        for i in range(2):
            tile = tile_of[block * 4 + half * 2 + i]
            lanes = pl.ds(pl.multiple_of(tile * 128, 128), 128)
            spread = jnp.zeros((128, 128), f32)
            for part, tokens in enumerate((own, partner)):
                rows = slice(part * SEQ, (part + 1) * SEQ)
                normed = tokens[:, lanes].astype(f32) * inverse[rows, :] * gain[:, lanes]
                total = jnp.sum(normed * back[rows, i * 128 : (i + 1) * 128], axis=0, keepdims=True)
                spread += jnp.where(row == 64 + members[part], total, 0.0)
            extra = spread.T
            spot = pl.multiple_of(jnp.minimum(tile, 4) * 128, 128)
            extra += jnp.where(tile < 5, out_cols[pl.ds(spot, 128), :], 0.0)
            here = slice(i * 128, (i + 1) * 128)
            result[here, :512] = part_grad[here, :512].astype(result.dtype)
            result[here, 512:] = (part_grad[here, 512:] + extra).astype(result.dtype)


def split_kernel(weight, spread):
    rows = weight[...]
    for core in range(2):
        cols = pad_lanes(group_columns(rows, core), LANES)
        for z in range(NZ):
            spread[2 * z + core, :, :] = cols


def exact_dot(values, picks):
    high = values.astype(bf16)
    rest = values - high.astype(f32)
    middle = rest.astype(bf16)
    low = (rest - middle.astype(f32)).astype(bf16)
    return dot(high, picks, 1, 0) + dot(middle, picks, 1, 0) + dot(low, picks, 1, 0)


def pack_kernel(pieces, grad_rows, packed):
    wide = pieces[...].astype(f32)
    sums = [sum(wide[2 * z + core] for z in range(NZ)) for core in range(2)]
    grads = whole_columns(*sums)
    grad_rows[...] = grads
    square = jnp.sum(jnp.sum(grads * grads, axis=1, keepdims=True), axis=0, keepdims=True)
    tails = [s[:, 512:] for s in sums]
    source = lax.broadcasted_iota(jnp.int32, (128, 128), 0)
    target = lax.broadcasted_iota(jnp.int32, (128, 128), 1)
    field = target // 8
    from_in = ((source == 64 + field) & (field < 4)).astype(bf16)
    from_zero = ((source == 64 + field) & (field >= 4) & (field < 8)).astype(bf16)
    from_one = ((source == 60 + field) & (field >= 8) & (field < 12)).astype(bf16)
    moved = (
        exact_dot(tails[0] + tails[1], from_in)
        + exact_dot(tails[0], from_zero)
        + exact_dot(tails[1], from_one)
    )
    row = lax.broadcasted_iota(jnp.int32, (8, 128), 0)
    lane = lax.broadcasted_iota(jnp.int32, (8, 128), 1)
    line = jnp.sum(jnp.where(row == (lane & 7), moved, 0.0), axis=0, keepdims=True)
    packed[...] = jnp.where(lane[:1] == 96, square, line)


def finish_kernel(
    everyone, grad_rows, weight_first, weight_second, in_first, in_second, out_first, out_second,
    weight_step, in_step, out_step,
):
    shares = everyone[...]
    lane = lax.broadcasted_iota(jnp.int32, (256, 128), 1)
    row = lax.broadcasted_iota(jnp.int32, (256, 128), 0)
    source = lax.broadcasted_iota(jnp.int32, (128, 128), 0)
    target = lax.broadcasted_iota(jnp.int32, (128, 128), 1)
    mine = (row & 15) == lane // 8
    fields = []
    for field in range(12):
        picks = (source == 8 * field + (target & 7)).astype(bf16)
        moved = jnp.where(mine, exact_dot(shares, picks), 0.0)
        fields.append(jnp.sum(moved.reshape(16, 16, 128), axis=1))

    def as_rows(start, tiles):
        return jnp.concatenate(
            [jnp.concatenate([f[t : t + 1] for t in range(tiles)], axis=1) for f in fields[start : start + 4]],
            axis=0,
        )

    in_grad = as_rows(0, TILES)
    out_grad = whole_columns(as_rows(4, 5), as_rows(8, 5))

    def total(values):
        return jnp.sum(jnp.sum(values, axis=1, keepdims=True), axis=0, keepdims=True)

    squared = (
        total(jnp.where(lane == 96, shares, 0.0)) + total(in_grad * in_grad) + total(out_grad * out_grad)
    )
    clip_scale = clip_limit / jnp.maximum(jnp.sqrt(squared), clip_limit)
    weight_step[...] = adam_direction(grad_rows[...], weight_first[...], weight_second[...], clip_scale)
    in_step[...] = adam_direction(in_grad, in_first[...], in_second[...], clip_scale)
    out_step[...] = adam_direction(out_grad, out_first[...], out_second[...], clip_scale)


SMEM = pl.BlockSpec(memory_space=pltpu.SMEM)
VMEM = pl.BlockSpec(memory_space=pltpu.VMEM)


def call(kernel, scalars, arrays, out_shape, name):
    single = not isinstance(out_shape, (list, tuple))
    return pl.pallas_call(
        kernel,
        in_specs=[SMEM] * len(scalars) + [VMEM] * len(arrays),
        out_specs=VMEM if single else [VMEM] * len(out_shape),
        out_shape=out_shape,
        name=name,
        compiler_params=pltpu.CompilerParams(vmem_limit_bytes=48 * 1024 * 1024),
    )(*scalars, *arrays)


def group_columns(array, group):
    pieces = [
        array[:, group * GROUP_Q : (group + 1) * GROUP_Q],
        array[:, 896 + group * 64 : 960 + group * 64],
        array[:, 1024 + group * 64 : 1088 + group * 64],
    ]
    return jnp.concatenate(pieces, axis=1)


def whole_columns(zero, one):
    return jnp.concatenate(
        [
            zero[:, :448],
            one[:, :448],
            zero[:, 448:512],
            one[:, 448:512],
            zero[:, 512:576],
            one[:, 512:576],
        ],
        axis=1,
    )


def pad_lanes(array, width):
    return jnp.pad(array, ((0, 0), (0, width - array.shape[1])))


def adam_direction(gradient, moment_one, moment_two, clip_scale):
    clipped = gradient * clip_scale
    first_new = beta_one * moment_one + (1.0 - beta_one) * clipped
    second_new = beta_two * moment_two + (1.0 - beta_two) * clipped * clipped
    first_hat = first_new / (1.0 - beta_one**step_number)
    second_hat = second_new / (1.0 - beta_two**step_number)
    return first_hat / (jnp.sqrt(second_hat) + adam_eps)


def per_device(
    tokens,
    member_ids,
    norm_gain,
    weight,
    qkv_bias,
    fast_in,
    fast_out,
    cotangent,
    weight_first,
    weight_second,
    in_first,
    in_second,
    out_first,
    out_second,
):
    here = lax.axis_index(AXIS)
    core = here % 2
    x_spot = (here // (2 * NZ)) % NX
    y_spot = here // (2 * NZ * NX)
    is_zero = core == 0

    spread = call(split_kernel, [], [weight], jax.ShapeDtypeStruct((2 * NZ, 8, LANES), bf16), "split")
    column = lax.all_to_all(
        spread, AXIS, split_axis=0, concat_axis=0, tiled=True, axis_index_groups=COLUMNS
    ).reshape(NZ * 16, LANES)
    column, tokens, cotangent, member_ids = lax.optimization_barrier(
        (column, tokens, cotangent, member_ids)
    )
    plane = jnp.concatenate([column] + [shift(column, INNER_RINGS, j) for j in (1, 2, 3)], axis=0)
    plane_a, plane_b = plane[:256], plane[256:]
    right_a = shift(plane_a, OUTER_RINGS, 1)
    left_b = shift(plane_b, OUTER_RINGS, -1)
    right_b = shift(plane_b, OUTER_RINGS, 1)
    left_a = shift(plane_a, OUTER_RINGS, -1)
    far_a = shift(right_a, OUTER_RINGS, 1)
    far_b = shift(left_b, OUTER_RINGS, -1)
    rows_of = [(plane_a, plane_b), (right_a, right_b), (far_a, far_b), (left_a, left_b)]

    partner_tokens = shift(tokens, PAIRS, 1)
    cot_zero = pad_lanes(cotangent[:, :GROUP_Q], 512)
    cot_one = pad_lanes(cotangent[:, GROUP_Q:], 512)
    cot_own = jnp.where(is_zero, cot_zero, cot_one)
    cot_partner = shift(jnp.where(is_zero, cot_one, cot_zero), PAIRS, 1)
    member_tile = jnp.broadcast_to(member_ids.astype(f32)[:, None], (8, 128))
    partner_member = shift(member_tile, PAIRS, 1)[0, 0].astype(jnp.int32)
    members = jnp.stack([member_ids[0], partner_member])
    pick = (members[:, None] == jnp.arange(4, dtype=jnp.int32)[None, :]).astype(f32)
    rates = jnp.sum(pick[:, :, None] * fast_in[None], axis=1)
    slopes_all = jnp.sum(pick[:, :, None] * fast_out[None], axis=1)
    slopes = pad_lanes(
        jnp.where(is_zero, group_columns(slopes_all, 0), group_columns(slopes_all, 1)), LANES
    )
    bias_all = qkv_bias[None, :]
    bias = pad_lanes(jnp.where(is_zero, group_columns(bias_all, 0), group_columns(bias_all, 1)), LANES)
    gain = norm_gain[None, :]
    cosine, sine = rope_tables()

    turn = jnp.arange(TILES, dtype=jnp.int32)
    outer, inner = turn // 4, turn % 4
    y_back = jnp.where(is_zero, outer, inner)
    x_back = jnp.where(is_zero, inner, outer)
    tile_of = ((y_spot - y_back) % NY) * NX + (x_spot - x_back) % NX

    scaled, inverse = call(
        scale_kernel,
        [tile_of],
        [tokens, partner_tokens, gain, rates],
        [
            jax.ShapeDtypeStruct((2 * SEQ, FEATURES), bf16),
            jax.ShapeDtypeStruct((2 * SEQ, 128), f32),
        ],
        "scale",
    )
    down, out_cols = call(
        attention_kernel,
        [members],
        [scaled, *[h for pair in rows_of for h in pair], slopes, bias, cosine, sine, cot_own, cot_partner],
        [
            jax.ShapeDtypeStruct((2 * SEQ, LANES), bf16),
            jax.ShapeDtypeStruct((LANES, 128), f32),
        ],
        "attention",
    )

    def block_grad(block):
        half = jax.ShapeDtypeStruct((256, LANES), f32 if block == 0 else bf16)
        return call(
            functools.partial(weight_kernel, block),
            [tile_of, members],
            [tokens, partner_tokens, gain, inverse, scaled, down, *rows_of[block], out_cols],
            [half, half],
            "weight_grad",
        )

    def added(left, right):
        return (left.astype(f32) + right.astype(f32)).astype(bf16)

    two_a, two_b = block_grad(2)
    left_far = shift(two_a, OUTER_RINGS, -1)
    right_far = shift(two_b, OUTER_RINGS, 1)
    one_a, one_b = block_grad(1)
    left_own = shift(one_b, OUTER_RINGS, -1)
    three_a, three_b = block_grad(3)
    right_own = shift(three_a, OUTER_RINGS, 1)
    zero_a, zero_b = block_grad(0)
    left_far, right_far, zero_a, zero_b = lax.optimization_barrier((left_far, right_far, zero_a, zero_b))
    left_sum = shift(added(one_a, left_far), OUTER_RINGS, -1)
    right_sum = shift(added(three_b, right_far), OUTER_RINGS, 1)
    sum_a = zero_a + right_own.astype(f32) + left_sum.astype(f32)
    sum_b = zero_b + left_own.astype(f32) + right_sum.astype(f32)
    parts = [sum_a[:128], sum_a[128:], sum_b[:128], sum_b[128:]]
    got = [shift(parts[j].astype(bf16), INNER_RINGS, -j) for j in (2, 1, 3)]
    column_sum = parts[0] + sum(g.astype(f32) for g in got)
    pieces = lax.all_to_all(
        column_sum.astype(bf16).reshape(2 * NZ, 8, LANES),
        AXIS,
        split_axis=0,
        concat_axis=0,
        tiled=True,
        axis_index_groups=COLUMNS,
    )
    grad_rows, packed = call(
        pack_kernel,
        [],
        [pieces],
        [jax.ShapeDtypeStruct((8, 1152), f32), jax.ShapeDtypeStruct((1, 128), f32)],
        "pack",
    )
    everyone = lax.all_to_all(
        jnp.broadcast_to(packed[:, None], (256, 1, 128)), AXIS, split_axis=0, concat_axis=0, tiled=True
    ).reshape(256, 128)
    return tuple(
        call(
            finish_kernel,
            [],
            [everyone, grad_rows, weight_first, weight_second, in_first, in_second, out_first, out_second],
            [
                jax.ShapeDtypeStruct((8, 1152), f32),
                jax.ShapeDtypeStruct((4, FEATURES), f32),
                jax.ShapeDtypeStruct((4, 1152), f32),
            ],
            "finish",
        )
    )


def solution(mesh):
    return jax.shard_map(
        per_device,
        mesh=mesh,
        in_specs=(
            P(AXIS, None),
            P(AXIS),
            P(),
            P(AXIS, None),
            P(),
            P(),
            P(),
            P(AXIS, None),
            P(AXIS, None),
            P(AXIS, None),
            P(),
            P(),
            P(),
            P(),
        ),
        out_specs=(P(AXIS, None), P(), P()),
        check_vma=False,
    )
```

```python
import math

import jax
import jax.numpy as jnp
from jax import lax
from jax.experimental import pallas as pl
from jax.experimental.pallas import tpu as pltpu
from jax.sharding import PartitionSpec as P


AXIS = "fsdp"
NY, NX, NZ = 4, 4, 8
HEAD_DIM = 64
GROUP_Q = 448
LANES = 640
SEQ = 128
FEATURES = 2048
TILES = FEATURES // 128

norm_eps = 1e-06
clip_limit = 1.0
beta_one = 0.9
beta_two = 0.95
adam_eps = 1e-08
rope_base = 1000000.0
step_number = 10.0


f32 = jnp.float32
bf16 = jnp.bfloat16


def device_of(y, x, z, c):
    return ((y * NX + x) * NZ + z) * 2 + c


COLUMNS = [
    [device_of(y, x, z, c) for z in range(NZ) for c in range(2)] for y in range(NY) for x in range(NX)
]
PAIRS = [
    [device_of(y, x, z, c) for c in range(2)] for y in range(NY) for x in range(NX) for z in range(NZ)
]
INNER_RINGS = [
    [device_of(y, x, z, 0) for x in range(NX)] for y in range(NY) for z in range(NZ)
] + [[device_of(y, x, z, 1) for y in range(NY)] for x in range(NX) for z in range(NZ)]
OUTER_RINGS = [
    [device_of(y, x, z, 0) for y in range(NY)] for x in range(NX) for z in range(NZ)
] + [[device_of(y, x, z, 1) for x in range(NX)] for y in range(NY) for z in range(NZ)]


def shift(array, rings, step):
    pairs = [(ring[i], ring[(i + step) % len(ring)]) for ring in rings for i in range(len(ring))]
    return lax.ppermute(array, AXIS, pairs)


def rope_tables():
    half_width = HEAD_DIM // 2
    spacing = jnp.arange(half_width, dtype=f32) * (2.0 / HEAD_DIM)
    frequency = jnp.exp(-math.log(rope_base) * spacing)
    angles = jnp.arange(SEQ, dtype=f32)[:, None] * frequency[None, :]
    cosine, sine = jnp.cos(angles), jnp.sin(angles)
    return (
        jnp.concatenate([cosine] * 4, axis=1),
        jnp.concatenate([-sine, sine, -sine, sine], axis=1),
    )


def dot(left, right, left_dim, right_dim):
    return lax.dot_general(
        left, right, (((left_dim,), (right_dim,)), ((), ())), preferred_element_type=f32
    )


def scale_kernel(tile_of, own, partner, gain, rates, *scaled):
    for part, tokens in enumerate((own, partner)):
        rows = slice(part * SEQ, (part + 1) * SEQ)
        wide = tokens[...].astype(f32)
        inv = lax.rsqrt(jnp.mean(wide * wide, axis=1, keepdims=True) + norm_eps)
        for i in range(TILES):
            lanes = pl.ds(pl.multiple_of(tile_of[i] * 128, 128), 128)
            normed = tokens[:, lanes].astype(f32) * inv * gain[:, lanes]
            spot = slice(i % 4 * 128, (i % 4 + 1) * 128)
            scaled[i // 4][rows, spot] = (normed * rates[part : part + 1, lanes]).astype(bf16)


def project_kernel(scaled0, scaled1, scaled3, near, right, left, partial):
    partial[...] = (
        dot(scaled0[...], near[...], 1, 0)
        + dot(scaled1[...], right[...], 1, 0)
        + dot(scaled3[...], left[...], 1, 0)
    )


def attention_kernel(
    members, scaled2, partial, far_a, far_b, slopes, bias, cosine_ref, sine_ref, cot_own, cot_partner, down
):
    cosine = cosine_ref[...]
    sine = sine_ref[...]
    lane = lax.broadcasted_iota(jnp.int32, (SEQ, 128), 1)
    row = lax.broadcasted_iota(jnp.int32, (SEQ, 128), 0)
    low = lane < 64
    first = (lane & 63) < 32
    causal = row >= lane
    score_scale = 1.0 / math.sqrt(HEAD_DIM)

    def swap(tile):
        return jnp.where(first, pltpu.roll(tile, 96, 1), pltpu.roll(tile, 32, 1))

    def half_turn(tile):
        return pltpu.roll(tile, 64, 1)

    projected = (
        partial[...]
        + dot(scaled2[:, :256], far_a[...], 1, 0)
        + dot(scaled2[:, 256:], far_b[...], 1, 0)
    )
    totals = []
    for part, cot in enumerate((cot_own, cot_partner)):
        rows = slice(part * SEQ, (part + 1) * SEQ)
        raw = projected[rows]
        slope = slopes[part : part + 1, :]
        biased = raw * slope + bias[...]
        turned = []
        for t in range(4):
            tile = biased[:, t * 128 : (t + 1) * 128]
            turned.append(tile * cosine + swap(tile) * sine)
        keys = turned[3]
        values = biased[:, 512:640]
        key_pair = jnp.concatenate(
            [jnp.where(low, half_turn(keys), 0.0), jnp.where(low, 0.0, keys)], axis=0
        ).astype(bf16)
        value_pair = jnp.concatenate(
            [jnp.where(low, values, 0.0), jnp.where(low, 0.0, half_turn(values))], axis=0
        ).astype(bf16)
        grads = []
        key_sum = jnp.zeros((2 * SEQ, 128), f32)
        value_sum = jnp.zeros((2 * SEQ, 128), f32)
        for t in range(4):
            query = turned[t].astype(bf16)
            upstream = cot[:, t * 128 : (t + 1) * 128]
            scores = dot(query, key_pair, 1, 1) * score_scale
            grad_probs = dot(upstream, value_pair, 1, 1)
            probs_bf, grads_bf = [], []
            for h in range(2):
                side = slice(h * SEQ, (h + 1) * SEQ)
                masked = jnp.where(causal, scores[:, side], -jnp.inf)
                raised = jnp.exp(masked - jnp.max(masked, axis=1, keepdims=True))
                probs = raised / jnp.sum(raised, axis=1, keepdims=True)
                gp = grad_probs[:, side]
                centre = jnp.sum(gp * probs, axis=1, keepdims=True)
                probs_bf.append(probs.astype(bf16))
                grads_bf.append((probs * (gp - centre) * score_scale).astype(bf16))
            probs_pair = jnp.concatenate(probs_bf, axis=1)
            grad_pair = jnp.concatenate(grads_bf, axis=1)
            grads.append(dot(grad_pair, key_pair, 1, 0))
            key_sum += dot(grad_pair, query, 0, 0)
            value_sum += dot(probs_pair, upstream, 0, 0)
        grad_key = jnp.where(low, 0.0, half_turn(key_sum[:SEQ]) + key_sum[SEQ:])
        grad_value = jnp.where(low, value_sum[:SEQ] + half_turn(value_sum[SEQ:]), 0.0)
        grads[3] = jnp.where(low, grads[3], grad_key)
        grads = [g * cosine - swap(g) * sine for g in grads] + [grad_value]
        grad_biased = jnp.concatenate(grads, axis=1)
        totals.append(jnp.sum(raw * grad_biased, axis=0, keepdims=True))
        down[rows, :] = (grad_biased * slope).astype(bf16)
    spread = jnp.zeros((SEQ, 128), f32)
    for part in range(2):
        for t in range(5):
            spread += jnp.where(
                row == 64 + 4 * t + members[part], totals[part][:, t * 128 : (t + 1) * 128], 0.0
            )
    spread = spread.T
    high = spread.astype(bf16).astype(f32)
    spread = high + pltpu.roll(spread - high, 20, 1)
    for part in range(2):
        rows = slice(part * SEQ, (part + 1) * SEQ)
        tail = jnp.where(lane == 127, members[part].astype(f32), 0.0)
        if part == 0:
            tail = jnp.where(lane == 127, tail, spread)
        last = down[rows, 512:640].astype(f32)
        down[rows, 512:640] = jnp.where(low, last, tail).astype(bf16)


def weight_terms(scaled, down, plane, carry):
    grads, totals, tails = carry
    back = dot(down, plane, 1, 1)
    grads = grads + dot(scaled, down, 0, 0)
    row = lax.broadcasted_iota(jnp.int32, (8, 512), 0)
    for part in range(scaled.shape[0] // SEQ):
        rows = slice(part * SEQ, (part + 1) * SEQ)
        member = down[part * SEQ : part * SEQ + 1, 639:640].astype(f32).astype(jnp.int32)
        total = jnp.sum(scaled[rows].astype(f32) * back[rows], axis=0, keepdims=True)
        totals = totals + jnp.where(row == member, total, 0.0)
    return grads, totals, tails


def near_kernel(scaled, down, plane, grads, totals, tails):
    zero = (jnp.zeros((512, LANES), f32), jnp.zeros((8, 512), f32), None)
    total = weight_terms(scaled[...], down[...], plane[...], zero)
    grads[...], totals[...] = total[:2]
    tails[...] = down[:SEQ, 512:].astype(f32)


def middle_kernel(
    scaled1, down1, scaled3, down3, plane, grads_in, totals_in, tails_in, grads, totals, tails
):
    total = (grads_in[...], totals_in[...], None)
    for scaled, down in ((scaled1, down1), (scaled3, down3)):
        total = weight_terms(scaled[...], down[...], plane[...], total)
    grads[...], totals[...] = total[:2]
    tails[...] = tails_in[...] + down1[:SEQ, 512:].astype(f32) + down3[:SEQ, 512:].astype(f32)


def last_kernel(
    tile_of, scaled, down_a, down_b, plane, grads_in, totals_in, tails_in, rates, part0, part1, part2, part3
):
    total = (grads_in[...], totals_in[...], None)
    total = weight_terms(scaled[:SEQ, :], down_a[...], plane[...], total)
    grads, totals, _ = weight_terms(scaled[SEQ:, :], down_b[...], plane[...], total)
    tails = tails_in[...] + down_a[:, 512:].astype(f32)
    tails = tails + pltpu.roll(tails, 108, 1)
    lane = lax.broadcasted_iota(jnp.int32, (SEQ, 128), 1)
    for i, result in enumerate((part0, part1, part2, part3)):
        tile = tile_of[i]
        here = slice(i * 128, (i + 1) * 128)
        shares = totals[:, here] / rates[:, pl.ds(pl.multiple_of(tile * 128, 128), 128)]
        extra = jnp.concatenate([jnp.zeros((64, 128), f32), shares, jnp.zeros((56, 128), f32)], axis=0).T
        for t in range(5):
            moved = pltpu.roll(tails, (4 - 4 * t) % 128, 1)
            extra = jnp.where((lane >= 68) & (lane < 72) & (tile == t), moved, extra)
        result[:, :512] = grads[here, :512].astype(result.dtype)
        result[:, 512:] = jnp.where(lane < 64, grads[here, 512:], extra).astype(result.dtype)


def split_kernel(weight, spread):
    rows = weight[...]
    for core in range(2):
        cols = pad_lanes(group_columns(rows, core), LANES)
        for z in range(NZ):
            spread[2 * z + core, :, :] = cols


def exact_dot(values, picks):
    high = values.astype(bf16)
    rest = values - high.astype(f32)
    middle = rest.astype(bf16)
    low = (rest - middle.astype(f32)).astype(bf16)
    return dot(high, picks, 1, 0) + dot(middle, picks, 1, 0) + dot(low, picks, 1, 0)


def pack_kernel(pieces, grad_rows, packed):
    wide = pieces[...].astype(f32)
    sums = [sum(wide[2 * z + core] for z in range(NZ)) for core in range(2)]
    grads = whole_columns(*sums)
    grad_rows[...] = grads
    square = jnp.sum(jnp.sum(grads * grads, axis=1, keepdims=True), axis=0, keepdims=True)
    tails = [s[:, 512:] for s in sums]
    source = lax.broadcasted_iota(jnp.int32, (128, 128), 0)
    target = lax.broadcasted_iota(jnp.int32, (128, 128), 1)
    field = target // 8
    from_in = ((source == 64 + field) & (field < 4)).astype(bf16)
    from_zero = ((source == 64 + field) & (field >= 4) & (field < 8)).astype(bf16)
    from_one = ((source == 60 + field) & (field >= 8) & (field < 12)).astype(bf16)
    moved = (
        exact_dot(tails[0] + tails[1], from_in)
        + exact_dot(tails[0], from_zero)
        + exact_dot(tails[1], from_one)
    )
    row = lax.broadcasted_iota(jnp.int32, (8, 128), 0)
    lane = lax.broadcasted_iota(jnp.int32, (8, 128), 1)
    line = jnp.sum(jnp.where(row == (lane & 7), moved, 0.0), axis=0, keepdims=True)
    packed[...] = jnp.where(lane[:1] == 96, square, line)


def finish_kernel(
    everyone, grad_rows, weight_first, weight_second, in_first, in_second, out_first, out_second,
    weight_step, in_step, out_step,
):
    shares = everyone[...]
    lane = lax.broadcasted_iota(jnp.int32, (256, 128), 1)
    row = lax.broadcasted_iota(jnp.int32, (256, 128), 0)
    source = lax.broadcasted_iota(jnp.int32, (128, 128), 0)
    target = lax.broadcasted_iota(jnp.int32, (128, 128), 1)
    mine = (row & 15) == lane // 8
    fields = []
    for field in range(12):
        picks = (source == 8 * field + (target & 7)).astype(bf16)
        moved = jnp.where(mine, exact_dot(shares, picks), 0.0)
        fields.append(jnp.sum(moved.reshape(16, 16, 128), axis=1))

    def as_rows(start, tiles):
        return jnp.concatenate(
            [jnp.concatenate([f[t : t + 1] for t in range(tiles)], axis=1) for f in fields[start : start + 4]],
            axis=0,
        )

    in_grad = as_rows(0, TILES)
    out_grad = whole_columns(as_rows(4, 5), as_rows(8, 5))

    def total(values):
        return jnp.sum(jnp.sum(values, axis=1, keepdims=True), axis=0, keepdims=True)

    squared = (
        total(jnp.where(lane == 96, shares, 0.0)) + total(in_grad * in_grad) + total(out_grad * out_grad)
    )
    clip_scale = clip_limit / jnp.maximum(jnp.sqrt(squared), clip_limit)
    weight_step[...] = adam_direction(grad_rows[...], weight_first[...], weight_second[...], clip_scale)
    in_step[...] = adam_direction(in_grad, in_first[...], in_second[...], clip_scale)
    out_step[...] = adam_direction(out_grad, out_first[...], out_second[...], clip_scale)


SMEM = pl.BlockSpec(memory_space=pltpu.SMEM)
VMEM = pl.BlockSpec(memory_space=pltpu.VMEM)


def call(kernel, scalars, arrays, out_shape):
    single = not isinstance(out_shape, (list, tuple))
    return pl.pallas_call(
        kernel,
        in_specs=[SMEM] * len(scalars) + [VMEM] * len(arrays),
        out_specs=VMEM if single else [VMEM] * len(out_shape),
        out_shape=out_shape,
        compiler_params=pltpu.CompilerParams(vmem_limit_bytes=48 * 1024 * 1024),
    )(*scalars, *arrays)


def group_columns(array, group):
    pieces = [
        array[:, group * GROUP_Q : (group + 1) * GROUP_Q],
        array[:, 896 + group * 64 : 960 + group * 64],
        array[:, 1024 + group * 64 : 1088 + group * 64],
    ]
    return jnp.concatenate(pieces, axis=1)


def whole_columns(zero, one):
    return jnp.concatenate(
        [
            zero[:, :448],
            one[:, :448],
            zero[:, 448:512],
            one[:, 448:512],
            zero[:, 512:576],
            one[:, 512:576],
        ],
        axis=1,
    )


def pad_lanes(array, width):
    return jnp.pad(array, ((0, 0), (0, width - array.shape[1])))


def adam_direction(gradient, moment_one, moment_two, clip_scale):
    clipped = gradient * clip_scale
    first_new = beta_one * moment_one + (1.0 - beta_one) * clipped
    second_new = beta_two * moment_two + (1.0 - beta_two) * clipped * clipped
    first_hat = first_new / (1.0 - beta_one**step_number)
    second_hat = second_new / (1.0 - beta_two**step_number)
    return first_hat / (jnp.sqrt(second_hat) + adam_eps)


def per_device(
    tokens,
    member_ids,
    norm_gain,
    weight,
    qkv_bias,
    fast_in,
    fast_out,
    cotangent,
    weight_first,
    weight_second,
    in_first,
    in_second,
    out_first,
    out_second,
):
    here = lax.axis_index(AXIS)
    core = here % 2
    x_spot = (here // (2 * NZ)) % NX
    y_spot = here // (2 * NZ * NX)
    is_zero = core == 0

    spread = call(split_kernel, [], [weight], jax.ShapeDtypeStruct((2 * NZ, 8, LANES), bf16))
    column = lax.all_to_all(
        spread, AXIS, split_axis=0, concat_axis=0, tiled=True, axis_index_groups=COLUMNS
    ).reshape(NZ * 16, LANES)
    column, tokens, cotangent, member_ids = lax.optimization_barrier(
        (column, tokens, cotangent, member_ids)
    )
    plane = jnp.concatenate([column] + [shift(column, INNER_RINGS, j) for j in (1, 2, 3)], axis=0)
    right = shift(plane, OUTER_RINGS, 1)
    left = shift(plane, OUTER_RINGS, -1)
    far_a = shift(right[:256], OUTER_RINGS, 1)
    far_b = shift(left[256:], OUTER_RINGS, -1)

    partner_tokens = shift(tokens, PAIRS, 1)
    cot_zero = pad_lanes(cotangent[:, :GROUP_Q], 512)
    cot_one = pad_lanes(cotangent[:, GROUP_Q:], 512)
    cot_own = jnp.where(is_zero, cot_zero, cot_one)
    cot_partner = shift(jnp.where(is_zero, cot_one, cot_zero), PAIRS, 1)
    member_tile = jnp.broadcast_to(member_ids.astype(f32)[:, None], (8, 128))
    partner_member = shift(member_tile, PAIRS, 1)[0, 0].astype(jnp.int32)
    members = jnp.stack([member_ids[0], partner_member])
    pick = (members[:, None] == jnp.arange(4, dtype=jnp.int32)[None, :]).astype(f32)
    rates = jnp.sum(pick[:, :, None] * fast_in[None], axis=1)
    slopes_all = jnp.sum(pick[:, :, None] * fast_out[None], axis=1)
    slopes = pad_lanes(
        jnp.where(is_zero, group_columns(slopes_all, 0), group_columns(slopes_all, 1)), LANES
    )
    bias_all = qkv_bias[None, :]
    bias = pad_lanes(jnp.where(is_zero, group_columns(bias_all, 0), group_columns(bias_all, 1)), LANES)
    gain = norm_gain[None, :]
    factors = jnp.concatenate([fast_in, jnp.ones((4, FEATURES), f32)])
    cosine, sine = rope_tables()

    turn = jnp.arange(TILES, dtype=jnp.int32)
    outer, inner = turn // 4, turn % 4
    y_back = jnp.where(is_zero, outer, inner)
    x_back = jnp.where(is_zero, inner, outer)
    tile_of = ((y_spot - y_back) % NY) * NX + (x_spot - x_back) % NX

    scaled = call(
        scale_kernel, [tile_of], [tokens, partner_tokens, gain, rates], [jax.ShapeDtypeStruct((2 * SEQ, 512), bf16)] * 4
    )
    partial = call(
        project_kernel,
        [],
        [scaled[0], scaled[1], scaled[3], plane, right, left],
        jax.ShapeDtypeStruct((2 * SEQ, LANES), f32),
    )
    far_scaled = [shift(scaled[j], OUTER_RINGS, -j) for j in (1, 2, 3)]
    down = call(
        attention_kernel,
        [members],
        [scaled[2], partial, far_a, far_b, slopes, bias, cosine, sine, cot_own, cot_partner],
        jax.ShapeDtypeStruct((2 * SEQ, LANES), bf16),
    )
    down_back = shift(down, OUTER_RINGS, 1)
    down_ahead = shift(down, OUTER_RINGS, -1)
    sums = [
        jax.ShapeDtypeStruct((512, LANES), f32),
        jax.ShapeDtypeStruct((8, 512), f32),
        jax.ShapeDtypeStruct((SEQ, 128), f32),
    ]
    near = call(near_kernel, [], [scaled[0], down, plane], sums)
    down_far_a = shift(down_back[:SEQ], OUTER_RINGS, 1)
    down_far_b = shift(down_ahead[SEQ:], OUTER_RINGS, -1)
    middle = call(middle_kernel, [], [far_scaled[0], down_ahead, far_scaled[2], down_back, plane, *near], sums)
    parts = call(
        last_kernel,
        [tile_of],
        [far_scaled[1], down_far_a, down_far_b, plane, *middle, factors],
        [jax.ShapeDtypeStruct((SEQ, LANES), f32)] + [jax.ShapeDtypeStruct((SEQ, LANES), bf16)] * 3,
    )
    got = [shift(parts[j], INNER_RINGS, -j) for j in (2, 1, 3)]
    column_sum = parts[0] + sum(g.astype(f32) for g in got)
    pieces = lax.all_to_all(
        column_sum.astype(bf16).reshape(2 * NZ, 8, LANES),
        AXIS,
        split_axis=0,
        concat_axis=0,
        tiled=True,
        axis_index_groups=COLUMNS,
    )
    grad_rows, packed = call(
        pack_kernel, [], [pieces], [jax.ShapeDtypeStruct((8, 1152), f32), jax.ShapeDtypeStruct((1, 128), f32)]
    )
    everyone = lax.all_to_all(
        jnp.broadcast_to(packed[:, None], (256, 1, 128)), AXIS, split_axis=0, concat_axis=0, tiled=True
    ).reshape(256, 128)
    return tuple(
        call(
            finish_kernel,
            [],
            [everyone, grad_rows, weight_first, weight_second, in_first, in_second, out_first, out_second],
            [
                jax.ShapeDtypeStruct((8, 1152), f32),
                jax.ShapeDtypeStruct((4, FEATURES), f32),
                jax.ShapeDtypeStruct((4, 1152), f32),
            ],
        )
    )


def solution(mesh):
    return jax.shard_map(
        per_device,
        mesh=mesh,
        in_specs=(
            P(AXIS, None),
            P(AXIS),
            P(),
            P(AXIS, None),
            P(),
            P(),
            P(),
            P(AXIS, None),
            P(AXIS, None),
            P(AXIS, None),
            P(),
            P(),
            P(),
            P(),
        ),
        out_specs=(P(AXIS, None), P(), P()),
        check_vma=False,
    )
```

```python
import functools
import math

import jax
import jax.numpy as jnp
from jax import lax
from jax.experimental import pallas as pl
from jax.experimental.pallas import tpu as pltpu
from jax.sharding import PartitionSpec as P


AXIS = "fsdp"
NY, NX, NZ = 4, 4, 8
HEAD_DIM = 64
GROUP_Q = 448
LANES = 640
SEQ = 128
FEATURES = 2048
TILES = FEATURES // 128

norm_eps = 1e-06
clip_limit = 1.0
beta_one = 0.9
beta_two = 0.95
adam_eps = 1e-08
rope_base = 1000000.0
step_number = 10.0


f32 = jnp.float32
bf16 = jnp.bfloat16


def device_of(y, x, z, c):
    return ((y * NX + x) * NZ + z) * 2 + c


COLUMNS = [
    [device_of(y, x, z, c) for z in range(NZ) for c in range(2)] for y in range(NY) for x in range(NX)
]
PAIRS = [
    [device_of(y, x, z, c) for c in range(2)] for y in range(NY) for x in range(NX) for z in range(NZ)
]
INNER_RINGS = [
    [device_of(y, x, z, 0) for x in range(NX)] for y in range(NY) for z in range(NZ)
] + [[device_of(y, x, z, 1) for y in range(NY)] for x in range(NX) for z in range(NZ)]
OUTER_RINGS = [
    [device_of(y, x, z, 0) for y in range(NY)] for x in range(NX) for z in range(NZ)
] + [[device_of(y, x, z, 1) for x in range(NX)] for y in range(NY) for z in range(NZ)]


def shift(array, rings, step):
    pairs = [(ring[i], ring[(i + step) % len(ring)]) for ring in rings for i in range(len(ring))]
    return lax.ppermute(array, AXIS, pairs)


def rope_tables():
    half_width = HEAD_DIM // 2
    spacing = jnp.arange(half_width, dtype=f32) * (2.0 / HEAD_DIM)
    frequency = jnp.exp(-math.log(rope_base) * spacing)
    angles = jnp.arange(SEQ, dtype=f32)[:, None] * frequency[None, :]
    cosine, sine = jnp.cos(angles), jnp.sin(angles)
    return (
        jnp.concatenate([cosine] * 4, axis=1),
        jnp.concatenate([-sine, sine, -sine, sine], axis=1),
    )


def dot(left, right, left_dim, right_dim):
    return lax.dot_general(
        left, right, (((left_dim,), (right_dim,)), ((), ())), preferred_element_type=f32
    )


def scale_kernel(tile_of, own, partner, gain, rates, *scaled):
    for part, tokens in enumerate((own, partner)):
        rows = slice(part * SEQ, (part + 1) * SEQ)
        wide = tokens[...].astype(f32)
        inv = lax.rsqrt(jnp.mean(wide * wide, axis=1, keepdims=True) + norm_eps)
        for i in range(TILES):
            lanes = pl.ds(pl.multiple_of(tile_of[i] * 128, 128), 128)
            normed = tokens[:, lanes].astype(f32) * inv * gain[:, lanes]
            spot = slice(i % 4 * 128, (i % 4 + 1) * 128)
            scaled[i // 4][rows, spot] = (normed * rates[part : part + 1, lanes]).astype(bf16)


def project_kernel(scaled0, scaled1, scaled3, near, right, left, partial):
    partial[...] = (
        dot(scaled0[...], near[...], 1, 0)
        + dot(scaled1[...], right[...], 1, 0)
        + dot(scaled3[...], left[...], 1, 0)
    )


def attention_kernel(
    part, members, scaled2, partial, far_a, far_b, slopes, bias, cosine_ref, sine_ref, cot, down
):
    cosine = cosine_ref[...]
    sine = sine_ref[...]
    lane = lax.broadcasted_iota(jnp.int32, (SEQ, 128), 1)
    row = lax.broadcasted_iota(jnp.int32, (SEQ, 128), 0)
    low = lane < 64
    first = (lane & 63) < 32
    causal = jnp.concatenate([row >= lane] * 4, axis=0)
    score_scale = 1.0 / math.sqrt(HEAD_DIM)

    def swap(tile):
        return jnp.where(first, pltpu.roll(tile, 96, 1), pltpu.roll(tile, 32, 1))

    def half_turn(tile):
        return pltpu.roll(tile, 64, 1)

    rows = slice(part * SEQ, (part + 1) * SEQ)
    raw = (
        partial[rows, :]
        + dot(scaled2[rows, :256], far_a[...], 1, 0)
        + dot(scaled2[rows, 256:], far_b[...], 1, 0)
    )
    slope = slopes[part : part + 1, :]
    biased = raw * slope + bias[...]
    turned = []
    for t in range(4):
        tile = biased[:, t * 128 : (t + 1) * 128]
        turned.append(tile * cosine + swap(tile) * sine)
    keys = turned[3]
    values = biased[:, 512:640]
    key_pair = jnp.concatenate(
        [jnp.where(low, half_turn(keys), 0.0), jnp.where(low, 0.0, keys)], axis=0
    ).astype(bf16)
    value_pair = jnp.concatenate(
        [jnp.where(low, values, 0.0), jnp.where(low, 0.0, half_turn(values))], axis=0
    ).astype(bf16)
    query = jnp.concatenate([q.astype(bf16) for q in turned], axis=0)
    upstream = jnp.concatenate([cot[:, t * 128 : (t + 1) * 128] for t in range(4)], axis=0)
    scores = dot(query, key_pair, 1, 1)
    grad_probs = dot(upstream, value_pair, 1, 1)
    probs_bf, grads_bf = [], []
    for h in range(2):
        side = slice(h * SEQ, (h + 1) * SEQ)
        masked = jnp.where(causal, scores[:, side] * score_scale, -jnp.inf)
        raised = jnp.exp(masked - jnp.max(masked, axis=1, keepdims=True))
        probs = raised * (1.0 / jnp.sum(raised, axis=1, keepdims=True))
        gp = grad_probs[:, side]
        centre = jnp.sum(gp * probs, axis=1, keepdims=True)
        probs_bf.append(probs.astype(bf16))
        grads_bf.append((probs * (gp - centre) * score_scale).astype(bf16))
    probs_pair = jnp.concatenate(probs_bf, axis=1)
    grad_pair = jnp.concatenate(grads_bf, axis=1)
    all_grads = dot(grad_pair, key_pair, 1, 0)
    key_sum = dot(grad_pair, query, 0, 0)
    value_sum = dot(probs_pair, upstream, 0, 0)
    grad_key = jnp.where(low, 0.0, half_turn(key_sum[:SEQ]) + key_sum[SEQ:])
    grad_value = jnp.where(low, value_sum[:SEQ] + half_turn(value_sum[SEQ:]), 0.0)
    grads = [all_grads[t * SEQ : (t + 1) * SEQ] for t in range(4)]
    grads[3] = jnp.where(low, grads[3], grad_key)
    grads = [g * cosine - swap(g) * sine for g in grads] + [grad_value]
    grad_biased = jnp.concatenate(grads, axis=1)
    total = jnp.sum(raw * grad_biased, axis=0, keepdims=True)
    member = members[part]
    spread = jnp.zeros((SEQ, 128), f32)
    for t in range(5):
        spread += jnp.where(row == 64 + 4 * t + member, total[:, t * 128 : (t + 1) * 128], 0.0)
    spread = spread.T
    high = spread.astype(bf16).astype(f32)
    spread = high + pltpu.roll(spread - high, 20, 1)
    tail = jnp.where(lane == 127, member.astype(f32), spread)
    grad_down = grad_biased * slope
    down[:, :512] = grad_down[:, :512].astype(bf16)
    down[:, 512:] = jnp.where(low, grad_down[:, 512:], tail).astype(bf16)


def weight_terms(scaled, down, plane, carry):
    grads, totals = carry
    back = dot(down, plane, 1, 1)
    grads = grads + dot(scaled, down, 0, 0)
    row = lax.broadcasted_iota(jnp.int32, (8, 512), 0)
    for part in range(scaled.shape[0] // SEQ):
        rows = slice(part * SEQ, (part + 1) * SEQ)
        member = down[part * SEQ : part * SEQ + 1, 639:640].astype(f32).astype(jnp.int32)
        total = jnp.sum(scaled[rows].astype(f32) * back[rows], axis=0, keepdims=True)
        totals = totals + jnp.where(row == member, total, 0.0)
    return grads, totals


def joined(first, second):
    return jnp.concatenate([first[...], second[...]], axis=0)


def tail_sum(*downs):
    return sum(down[:, 512:].astype(f32) for down in downs)


def near_kernel(scaled, down0, down1, plane, grads, totals, tails):
    zero = (jnp.zeros((512, LANES), f32), jnp.zeros((8, 512), f32))
    grads[...], totals[...] = weight_terms(scaled[...], joined(down0, down1), plane[...], zero)
    tails[...] = tail_sum(down0, down1)


def middle_kernel(
    scaled1, ahead0, ahead1, scaled3, back0, back1, plane, grads_in, totals_in, tails_in, grads, totals, tails
):
    total = (grads_in[...], totals_in[...])
    total = weight_terms(scaled1[...], joined(ahead0, ahead1), plane[...], total)
    grads[...], totals[...] = weight_terms(scaled3[...], joined(back0, back1), plane[...], total)
    tails[...] = tails_in[...] + tail_sum(ahead0, ahead1, back0, back1)


def last_kernel(
    tile_of, scaled, down_a, down_b, plane, grads_in, totals_in, tails_in, rates, part0, part1, part2, part3
):
    total = (grads_in[...], totals_in[...])
    grads, totals = weight_terms(scaled[...], joined(down_a, down_b), plane[...], total)
    tails = tails_in[...] + tail_sum(down_a, down_b)
    tails = tails + pltpu.roll(tails, 108, 1)
    lane = lax.broadcasted_iota(jnp.int32, (SEQ, 128), 1)
    for i, result in enumerate((part0, part1, part2, part3)):
        tile = tile_of[i]
        here = slice(i * 128, (i + 1) * 128)
        shares = totals[:, here] / rates[:, pl.ds(pl.multiple_of(tile * 128, 128), 128)]
        extra = jnp.concatenate([jnp.zeros((64, 128), f32), shares, jnp.zeros((56, 128), f32)], axis=0).T
        for t in range(5):
            moved = pltpu.roll(tails, (4 - 4 * t) % 128, 1)
            extra = jnp.where((lane >= 68) & (lane < 72) & (tile == t), moved, extra)
        result[:, :512] = grads[here, :512].astype(result.dtype)
        result[:, 512:] = jnp.where(lane < 64, grads[here, 512:], extra).astype(result.dtype)


def split_kernel(weight, spread):
    rows = weight[...]
    for core in range(2):
        cols = pad_lanes(group_columns(rows, core), LANES)
        for z in range(NZ):
            spread[2 * z + core, :, :] = cols


def exact_dot(values, picks):
    high = values.astype(bf16)
    rest = values - high.astype(f32)
    middle = rest.astype(bf16)
    low = (rest - middle.astype(f32)).astype(bf16)
    return dot(high, picks, 1, 0) + dot(middle, picks, 1, 0) + dot(low, picks, 1, 0)


def pack_kernel(pieces, grad_rows, packed):
    wide = pieces[...].astype(f32)
    sums = [sum(wide[2 * z + core] for z in range(NZ)) for core in range(2)]
    grads = whole_columns(*sums)
    grad_rows[...] = grads
    square = jnp.sum(jnp.sum(grads * grads, axis=1, keepdims=True), axis=0, keepdims=True)
    tails = [s[:, 512:] for s in sums]
    source = lax.broadcasted_iota(jnp.int32, (128, 128), 0)
    target = lax.broadcasted_iota(jnp.int32, (128, 128), 1)
    field = target // 8
    from_in = ((source == 64 + field) & (field < 4)).astype(bf16)
    from_zero = ((source == 64 + field) & (field >= 4) & (field < 8)).astype(bf16)
    from_one = ((source == 60 + field) & (field >= 8) & (field < 12)).astype(bf16)
    moved = (
        exact_dot(tails[0] + tails[1], from_in)
        + exact_dot(tails[0], from_zero)
        + exact_dot(tails[1], from_one)
    )
    row = lax.broadcasted_iota(jnp.int32, (8, 128), 0)
    lane = lax.broadcasted_iota(jnp.int32, (8, 128), 1)
    line = jnp.sum(jnp.where(row == (lane & 7), moved, 0.0), axis=0, keepdims=True)
    packed[...] = jnp.where(lane[:1] == 96, square, line)


def finish_kernel(
    everyone, grad_rows, weight_first, weight_second, in_first, in_second, out_first, out_second,
    weight_step, in_step, out_step,
):
    shares = everyone[...]
    lane = lax.broadcasted_iota(jnp.int32, (256, 128), 1)
    row = lax.broadcasted_iota(jnp.int32, (256, 128), 0)
    source = lax.broadcasted_iota(jnp.int32, (128, 128), 0)
    target = lax.broadcasted_iota(jnp.int32, (128, 128), 1)
    mine = (row & 15) == lane // 8
    fields = []
    for field in range(12):
        picks = (source == 8 * field + (target & 7)).astype(bf16)
        moved = jnp.where(mine, exact_dot(shares, picks), 0.0)
        fields.append(jnp.sum(moved.reshape(16, 16, 128), axis=1))

    def as_rows(start, tiles):
        return jnp.concatenate(
            [jnp.concatenate([f[t : t + 1] for t in range(tiles)], axis=1) for f in fields[start : start + 4]],
            axis=0,
        )

    in_grad = as_rows(0, TILES)
    out_grad = whole_columns(as_rows(4, 5), as_rows(8, 5))

    def total(values):
        return jnp.sum(jnp.sum(values, axis=1, keepdims=True), axis=0, keepdims=True)

    squared = (
        total(jnp.where(lane == 96, shares, 0.0)) + total(in_grad * in_grad) + total(out_grad * out_grad)
    )
    clip_scale = clip_limit / jnp.maximum(jnp.sqrt(squared), clip_limit)
    weight_step[...] = adam_direction(grad_rows[...], weight_first[...], weight_second[...], clip_scale)
    in_step[...] = adam_direction(in_grad, in_first[...], in_second[...], clip_scale)
    out_step[...] = adam_direction(out_grad, out_first[...], out_second[...], clip_scale)


SMEM = pl.BlockSpec(memory_space=pltpu.SMEM)
VMEM = pl.BlockSpec(memory_space=pltpu.VMEM)


def call(kernel, scalars, arrays, out_shape):
    single = not isinstance(out_shape, (list, tuple))
    return pl.pallas_call(
        kernel,
        in_specs=[SMEM] * len(scalars) + [VMEM] * len(arrays),
        out_specs=VMEM if single else [VMEM] * len(out_shape),
        out_shape=out_shape,
        compiler_params=pltpu.CompilerParams(vmem_limit_bytes=48 * 1024 * 1024),
    )(*scalars, *arrays)


def group_columns(array, group):
    pieces = [
        array[:, group * GROUP_Q : (group + 1) * GROUP_Q],
        array[:, 896 + group * 64 : 960 + group * 64],
        array[:, 1024 + group * 64 : 1088 + group * 64],
    ]
    return jnp.concatenate(pieces, axis=1)


def whole_columns(zero, one):
    return jnp.concatenate(
        [
            zero[:, :448],
            one[:, :448],
            zero[:, 448:512],
            one[:, 448:512],
            zero[:, 512:576],
            one[:, 512:576],
        ],
        axis=1,
    )


def pad_lanes(array, width):
    return jnp.pad(array, ((0, 0), (0, width - array.shape[1])))


def adam_direction(gradient, moment_one, moment_two, clip_scale):
    clipped = gradient * clip_scale
    first_new = beta_one * moment_one + (1.0 - beta_one) * clipped
    second_new = beta_two * moment_two + (1.0 - beta_two) * clipped * clipped
    first_hat = first_new / (1.0 - beta_one**step_number)
    second_hat = second_new / (1.0 - beta_two**step_number)
    return first_hat / (jnp.sqrt(second_hat) + adam_eps)


def per_device(
    tokens,
    member_ids,
    norm_gain,
    weight,
    qkv_bias,
    fast_in,
    fast_out,
    cotangent,
    weight_first,
    weight_second,
    in_first,
    in_second,
    out_first,
    out_second,
):
    here = lax.axis_index(AXIS)
    core = here % 2
    x_spot = (here // (2 * NZ)) % NX
    y_spot = here // (2 * NZ * NX)
    is_zero = core == 0

    spread = call(split_kernel, [], [weight], jax.ShapeDtypeStruct((2 * NZ, 8, LANES), bf16))
    column = lax.all_to_all(
        spread, AXIS, split_axis=0, concat_axis=0, tiled=True, axis_index_groups=COLUMNS
    ).reshape(NZ * 16, LANES)
    column, tokens, cotangent, member_ids = lax.optimization_barrier(
        (column, tokens, cotangent, member_ids)
    )
    plane = jnp.concatenate([column] + [shift(column, INNER_RINGS, j) for j in (1, 2, 3)], axis=0)
    right = shift(plane, OUTER_RINGS, 1)
    left = shift(plane, OUTER_RINGS, -1)
    far_a = shift(right[:256], OUTER_RINGS, 1)
    far_b = shift(left[256:], OUTER_RINGS, -1)

    partner_tokens = shift(tokens, PAIRS, 1)
    cot_zero = pad_lanes(cotangent[:, :GROUP_Q], 512)
    cot_one = pad_lanes(cotangent[:, GROUP_Q:], 512)
    cot_own = jnp.where(is_zero, cot_zero, cot_one)
    cot_partner = shift(jnp.where(is_zero, cot_one, cot_zero), PAIRS, 1)
    member_tile = jnp.broadcast_to(member_ids.astype(f32)[:, None], (8, 128))
    partner_member = shift(member_tile, PAIRS, 1)[0, 0].astype(jnp.int32)
    members = jnp.stack([member_ids[0], partner_member])
    pick = (members[:, None] == jnp.arange(4, dtype=jnp.int32)[None, :]).astype(f32)
    rates = jnp.sum(pick[:, :, None] * fast_in[None], axis=1)
    slopes_all = jnp.sum(pick[:, :, None] * fast_out[None], axis=1)
    slopes = pad_lanes(
        jnp.where(is_zero, group_columns(slopes_all, 0), group_columns(slopes_all, 1)), LANES
    )
    bias_all = qkv_bias[None, :]
    bias = pad_lanes(jnp.where(is_zero, group_columns(bias_all, 0), group_columns(bias_all, 1)), LANES)
    gain = norm_gain[None, :]
    factors = jnp.concatenate([fast_in, jnp.ones((4, FEATURES), f32)])
    cosine, sine = rope_tables()

    turn = jnp.arange(TILES, dtype=jnp.int32)
    outer, inner = turn // 4, turn % 4
    y_back = jnp.where(is_zero, outer, inner)
    x_back = jnp.where(is_zero, inner, outer)
    tile_of = ((y_spot - y_back) % NY) * NX + (x_spot - x_back) % NX

    scaled = call(
        scale_kernel, [tile_of], [tokens, partner_tokens, gain, rates], [jax.ShapeDtypeStruct((2 * SEQ, 512), bf16)] * 4
    )
    partial = call(
        project_kernel,
        [],
        [scaled[0], scaled[1], scaled[3], plane, right, left],
        jax.ShapeDtypeStruct((2 * SEQ, LANES), f32),
    )
    far_scaled = [shift(scaled[j], OUTER_RINGS, -j) for j in (1, 2, 3)]
    downs, backs, aheads = [], [], []
    for part, cot in enumerate((cot_own, cot_partner)):
        downs.append(
            call(
                functools.partial(attention_kernel, part),
                [members],
                [scaled[2], partial, far_a, far_b, slopes, bias, cosine, sine, cot],
                jax.ShapeDtypeStruct((SEQ, LANES), bf16),
            )
        )
        backs.append(shift(downs[part], OUTER_RINGS, 1))
        aheads.append(shift(downs[part], OUTER_RINGS, -1))
    sums = [
        jax.ShapeDtypeStruct((512, LANES), f32),
        jax.ShapeDtypeStruct((8, 512), f32),
        jax.ShapeDtypeStruct((SEQ, 128), f32),
    ]
    near = call(near_kernel, [], [scaled[0], *downs, plane], sums)
    down_far_a = shift(backs[0], OUTER_RINGS, 1)
    down_far_b = shift(aheads[1], OUTER_RINGS, -1)
    middle = call(middle_kernel, [], [far_scaled[0], *aheads, far_scaled[2], *backs, plane, *near], sums)
    parts = call(
        last_kernel,
        [tile_of],
        [far_scaled[1], down_far_a, down_far_b, plane, *middle, factors],
        [jax.ShapeDtypeStruct((SEQ, LANES), f32)] + [jax.ShapeDtypeStruct((SEQ, LANES), bf16)] * 3,
    )
    got = [shift(parts[j], INNER_RINGS, -j) for j in (2, 1, 3)]
    column_sum = parts[0] + sum(g.astype(f32) for g in got)
    pieces = lax.all_to_all(
        column_sum.astype(bf16).reshape(2 * NZ, 8, LANES),
        AXIS,
        split_axis=0,
        concat_axis=0,
        tiled=True,
        axis_index_groups=COLUMNS,
    )
    grad_rows, packed = call(
        pack_kernel, [], [pieces], [jax.ShapeDtypeStruct((8, 1152), f32), jax.ShapeDtypeStruct((1, 128), f32)]
    )
    everyone = lax.all_to_all(
        jnp.broadcast_to(packed[:, None], (256, 1, 128)), AXIS, split_axis=0, concat_axis=0, tiled=True
    ).reshape(256, 128)
    return tuple(
        call(
            finish_kernel,
            [],
            [everyone, grad_rows, weight_first, weight_second, in_first, in_second, out_first, out_second],
            [
                jax.ShapeDtypeStruct((8, 1152), f32),
                jax.ShapeDtypeStruct((4, FEATURES), f32),
                jax.ShapeDtypeStruct((4, 1152), f32),
            ],
        )
    )


def solution(mesh):
    return jax.shard_map(
        per_device,
        mesh=mesh,
        in_specs=(
            P(AXIS, None),
            P(AXIS),
            P(),
            P(AXIS, None),
            P(),
            P(),
            P(),
            P(AXIS, None),
            P(AXIS, None),
            P(AXIS, None),
            P(),
            P(),
            P(),
            P(),
        ),
        out_specs=(P(AXIS, None), P(), P()),
        check_vma=False,
    )
```

```python
import math

import jax
import jax.numpy as jnp
from jax import lax
from jax.experimental import pallas as pl
from jax.experimental.pallas import tpu as pltpu
from jax.sharding import PartitionSpec as P


AXIS = "fsdp"
NY, NX, NZ = 4, 4, 8
HEAD_DIM = 64
GROUP_Q = 448
LANES = 640
SEQ = 128
FEATURES = 2048
TILES = FEATURES // 128

norm_eps = 1e-06
clip_limit = 1.0
beta_one = 0.9
beta_two = 0.95
adam_eps = 1e-08
rope_base = 1000000.0
step_number = 10.0


f32 = jnp.float32
bf16 = jnp.bfloat16


def device_of(y, x, z, c):
    return ((y * NX + x) * NZ + z) * 2 + c


COLUMNS = [
    [device_of(y, x, z, c) for z in range(NZ) for c in range(2)] for y in range(NY) for x in range(NX)
]
PAIRS = [
    [device_of(y, x, z, c) for c in range(2)] for y in range(NY) for x in range(NX) for z in range(NZ)
]
INNER_RINGS = [
    [device_of(y, x, z, 0) for x in range(NX)] for y in range(NY) for z in range(NZ)
] + [[device_of(y, x, z, 1) for y in range(NY)] for x in range(NX) for z in range(NZ)]
OUTER_RINGS = [
    [device_of(y, x, z, 0) for y in range(NY)] for x in range(NX) for z in range(NZ)
] + [[device_of(y, x, z, 1) for x in range(NX)] for y in range(NY) for z in range(NZ)]


def shift(array, rings, step):
    pairs = [(ring[i], ring[(i + step) % len(ring)]) for ring in rings for i in range(len(ring))]
    return lax.ppermute(array, AXIS, pairs)


def rope_tables():
    half_width = HEAD_DIM // 2
    spacing = jnp.arange(half_width, dtype=f32) * (2.0 / HEAD_DIM)
    frequency = jnp.exp(-math.log(rope_base) * spacing)
    angles = jnp.arange(SEQ, dtype=f32)[:, None] * frequency[None, :]
    cosine, sine = jnp.cos(angles), jnp.sin(angles)
    return (
        jnp.concatenate([cosine] * 4, axis=1),
        jnp.concatenate([-sine, sine, -sine, sine], axis=1),
    )


def dot(left, right, left_dim, right_dim):
    return lax.dot_general(
        left, right, (((left_dim,), (right_dim,)), ((), ())), preferred_element_type=f32
    )


def scale_kernel(tile_of, own, partner, gain, rates, *scaled):
    for part, tokens in enumerate((own, partner)):
        rows = slice(part * SEQ, (part + 1) * SEQ)
        wide = tokens[...].astype(f32)
        inv = lax.rsqrt(jnp.mean(wide * wide, axis=1, keepdims=True) + norm_eps)
        for i in range(TILES):
            lanes = pl.ds(pl.multiple_of(tile_of[i] * 128, 128), 128)
            normed = tokens[:, lanes].astype(f32) * inv * gain[:, lanes]
            spot = slice(i % 4 * 128, (i % 4 + 1) * 128)
            scaled[i // 4][rows, spot] = (normed * rates[part : part + 1, lanes]).astype(bf16)


def project_kernel(scaled0, scaled1, scaled3, *refs):
    halves, partial = refs[:-1], refs[-1]
    partial[...] = sum(
        dot(scaled[:, half * 256 : (half + 1) * 256], halves[2 * j + half][...], 1, 0)
        for j, scaled in enumerate((scaled0, scaled1, scaled3))
        for half in range(2)
    )


def attention_kernel(
    members, scaled2, partial, far_a, far_b, slopes, bias, cosine_ref, sine_ref, cot_own, cot_partner, down
):
    cosine = cosine_ref[...]
    sine = sine_ref[...]
    lane = lax.broadcasted_iota(jnp.int32, (SEQ, 128), 1)
    row = lax.broadcasted_iota(jnp.int32, (SEQ, 128), 0)
    low = lane < 64
    first = (lane & 63) < 32
    causal = jnp.concatenate([row >= lane] * 4, axis=0)
    score_scale = 1.0 / math.sqrt(HEAD_DIM)

    def swap(tile):
        return jnp.where(first, pltpu.roll(tile, 96, 1), pltpu.roll(tile, 32, 1))

    def half_turn(tile):
        return pltpu.roll(tile, 64, 1)

    projected = (
        partial[...]
        + dot(scaled2[:, :256], far_a[...], 1, 0)
        + dot(scaled2[:, 256:], far_b[...], 1, 0)
    )
    totals = []
    for part, cot in enumerate((cot_own, cot_partner)):
        rows = slice(part * SEQ, (part + 1) * SEQ)
        raw = projected[rows]
        slope = slopes[part : part + 1, :]
        biased = raw * slope + bias[...]
        turned = []
        for t in range(4):
            tile = biased[:, t * 128 : (t + 1) * 128]
            turned.append(tile * cosine + swap(tile) * sine)
        keys = turned[3]
        values = biased[:, 512:640]
        key_pair = jnp.concatenate(
            [jnp.where(low, half_turn(keys), 0.0), jnp.where(low, 0.0, keys)], axis=0
        ).astype(bf16)
        value_pair = jnp.concatenate(
            [jnp.where(low, values, 0.0), jnp.where(low, 0.0, half_turn(values))], axis=0
        ).astype(bf16)
        query = jnp.concatenate([q.astype(bf16) for q in turned], axis=0)
        upstream = jnp.concatenate([cot[:, t * 128 : (t + 1) * 128] for t in range(4)], axis=0)
        scores = dot(query, key_pair, 1, 1)
        grad_probs = dot(upstream, value_pair, 1, 1)
        probs_bf, grads_bf = [], []
        for h in range(2):
            side = slice(h * SEQ, (h + 1) * SEQ)
            masked = jnp.where(causal, scores[:, side] * score_scale, -jnp.inf)
            raised = jnp.exp(masked - jnp.max(masked, axis=1, keepdims=True))
            probs = raised * (1.0 / jnp.sum(raised, axis=1, keepdims=True))
            gp = grad_probs[:, side]
            centre = jnp.sum(gp * probs, axis=1, keepdims=True)
            probs_bf.append(probs.astype(bf16))
            grads_bf.append((probs * (gp - centre) * score_scale).astype(bf16))
        probs_pair = jnp.concatenate(probs_bf, axis=1)
        grad_pair = jnp.concatenate(grads_bf, axis=1)
        all_grads = dot(grad_pair, key_pair, 1, 0)
        key_sum = dot(grad_pair, query, 0, 0)
        value_sum = dot(probs_pair, upstream, 0, 0)
        grad_key = jnp.where(low, 0.0, half_turn(key_sum[:SEQ]) + key_sum[SEQ:])
        grad_value = jnp.where(low, value_sum[:SEQ] + half_turn(value_sum[SEQ:]), 0.0)
        grads = [all_grads[t * SEQ : (t + 1) * SEQ] for t in range(4)]
        grads[3] = jnp.where(low, grads[3], grad_key)
        grads = [g * cosine - swap(g) * sine for g in grads] + [grad_value]
        grad_biased = jnp.concatenate(grads, axis=1)
        totals.append(jnp.sum(raw * grad_biased, axis=0, keepdims=True))
        down[rows, :] = (grad_biased * slope).astype(bf16)
    spread = jnp.zeros((SEQ, 128), f32)
    for part in range(2):
        for t in range(5):
            spread += jnp.where(
                row == 64 + 4 * t + members[part], totals[part][:, t * 128 : (t + 1) * 128], 0.0
            )
    spread = spread.T
    high = spread.astype(bf16).astype(f32)
    spread = high + pltpu.roll(spread - high, 20, 1)
    for part in range(2):
        rows = slice(part * SEQ, (part + 1) * SEQ)
        tail = jnp.where(lane == 127, members[part].astype(f32), 0.0)
        if part == 0:
            tail = jnp.where(lane == 127, tail, spread)
        last = down[rows, 512:640].astype(f32)
        down[rows, 512:640] = jnp.where(low, last, tail).astype(bf16)


def weight_terms(scaled, down, planes, carry):
    grads, totals, tails = carry
    back = jnp.concatenate([dot(down, plane[...], 1, 1) for plane in planes], axis=1)
    grads = grads + dot(scaled, down, 0, 0)
    row = lax.broadcasted_iota(jnp.int32, (8, 512), 0)
    for part in range(scaled.shape[0] // SEQ):
        rows = slice(part * SEQ, (part + 1) * SEQ)
        member = down[part * SEQ : part * SEQ + 1, 639:640].astype(f32).astype(jnp.int32)
        total = jnp.sum(scaled[rows].astype(f32) * back[rows], axis=0, keepdims=True)
        totals = totals + jnp.where(row == member, total, 0.0)
    return grads, totals, tails


def near_kernel(scaled, down, plane_a, plane_b, grads, totals, tails):
    zero = (jnp.zeros((512, LANES), f32), jnp.zeros((8, 512), f32), None)
    total = weight_terms(scaled[...], down[...], (plane_a, plane_b), zero)
    grads[...], totals[...] = total[:2]
    tails[...] = down[:SEQ, 512:].astype(f32)


def middle_kernel(
    scaled1, down1, scaled3, down3, plane_a, plane_b, grads_in, totals_in, tails_in, grads, totals, tails
):
    total = (grads_in[...], totals_in[...], None)
    for scaled, down in ((scaled1, down1), (scaled3, down3)):
        total = weight_terms(scaled[...], down[...], (plane_a, plane_b), total)
    grads[...], totals[...] = total[:2]
    tails[...] = tails_in[...] + down1[:SEQ, 512:].astype(f32) + down3[:SEQ, 512:].astype(f32)


def last_kernel(
    tile_of, scaled, down_a, down_b, plane_a, plane_b, grads_in, totals_in, tails_in, rates, *parts
):
    total = (grads_in[...], totals_in[...], None)
    down = jnp.concatenate([down_a[...], down_b[...]], axis=0)
    grads, totals, _ = weight_terms(scaled[...], down, (plane_a, plane_b), total)
    tails = tails_in[...] + down_a[:, 512:].astype(f32)
    tails = tails + pltpu.roll(tails, 108, 1)
    lane = lax.broadcasted_iota(jnp.int32, (SEQ, 128), 1)
    for i, result in enumerate(parts):
        tile = tile_of[i]
        here = slice(i * 128, (i + 1) * 128)
        shares = totals[:, here] / rates[:, pl.ds(pl.multiple_of(tile * 128, 128), 128)]
        extra = jnp.concatenate([jnp.zeros((64, 128), f32), shares, jnp.zeros((56, 128), f32)], axis=0).T
        for t in range(5):
            moved = pltpu.roll(tails, (4 - 4 * t) % 128, 1)
            extra = jnp.where((lane >= 68) & (lane < 72) & (tile == t), moved, extra)
        result[:, :512] = grads[here, :512].astype(result.dtype)
        result[:, 512:] = jnp.where(lane < 64, grads[here, 512:], extra).astype(result.dtype)


def split_kernel(weight, spread):
    rows = weight[...]
    for core in range(2):
        cols = pad_lanes(group_columns(rows, core), LANES)
        for z in range(NZ):
            spread[2 * z + core, :, :] = cols


def exact_dot(values, picks):
    high = values.astype(bf16)
    rest = values - high.astype(f32)
    middle = rest.astype(bf16)
    low = (rest - middle.astype(f32)).astype(bf16)
    return dot(high, picks, 1, 0) + dot(middle, picks, 1, 0) + dot(low, picks, 1, 0)


def pack_kernel(pieces, grad_rows, packed):
    wide = pieces[...].astype(f32)
    sums = [sum(wide[2 * z + core] for z in range(NZ)) for core in range(2)]
    grads = whole_columns(*sums)
    grad_rows[...] = grads
    square = jnp.sum(jnp.sum(grads * grads, axis=1, keepdims=True), axis=0, keepdims=True)
    tails = [s[:, 512:] for s in sums]
    source = lax.broadcasted_iota(jnp.int32, (128, 128), 0)
    target = lax.broadcasted_iota(jnp.int32, (128, 128), 1)
    field = target // 8
    from_in = ((source == 64 + field) & (field < 4)).astype(bf16)
    from_zero = ((source == 64 + field) & (field >= 4) & (field < 8)).astype(bf16)
    from_one = ((source == 60 + field) & (field >= 8) & (field < 12)).astype(bf16)
    moved = (
        exact_dot(tails[0] + tails[1], from_in)
        + exact_dot(tails[0], from_zero)
        + exact_dot(tails[1], from_one)
    )
    row = lax.broadcasted_iota(jnp.int32, (8, 128), 0)
    lane = lax.broadcasted_iota(jnp.int32, (8, 128), 1)
    line = jnp.sum(jnp.where(row == (lane & 7), moved, 0.0), axis=0, keepdims=True)
    packed[...] = jnp.where(lane[:1] == 96, square, line)


def finish_kernel(
    everyone, grad_rows, weight_first, weight_second, in_first, in_second, out_first, out_second,
    weight_step, in_step, out_step,
):
    shares = everyone[...]
    lane = lax.broadcasted_iota(jnp.int32, (256, 128), 1)
    row = lax.broadcasted_iota(jnp.int32, (256, 128), 0)
    source = lax.broadcasted_iota(jnp.int32, (128, 128), 0)
    target = lax.broadcasted_iota(jnp.int32, (128, 128), 1)
    mine = (row & 15) == lane // 8
    fields = []
    for field in range(12):
        picks = (source == 8 * field + (target & 7)).astype(bf16)
        moved = jnp.where(mine, exact_dot(shares, picks), 0.0)
        fields.append(jnp.sum(moved.reshape(16, 16, 128), axis=1))

    def as_rows(start, tiles):
        return jnp.concatenate(
            [jnp.concatenate([f[t : t + 1] for t in range(tiles)], axis=1) for f in fields[start : start + 4]],
            axis=0,
        )

    in_grad = as_rows(0, TILES)
    out_grad = whole_columns(as_rows(4, 5), as_rows(8, 5))

    def total(values):
        return jnp.sum(jnp.sum(values, axis=1, keepdims=True), axis=0, keepdims=True)

    squared = (
        total(jnp.where(lane == 96, shares, 0.0)) + total(in_grad * in_grad) + total(out_grad * out_grad)
    )
    clip_scale = clip_limit / jnp.maximum(jnp.sqrt(squared), clip_limit)
    weight_step[...] = adam_direction(grad_rows[...], weight_first[...], weight_second[...], clip_scale)
    in_step[...] = adam_direction(in_grad, in_first[...], in_second[...], clip_scale)
    out_step[...] = adam_direction(out_grad, out_first[...], out_second[...], clip_scale)


SMEM = pl.BlockSpec(memory_space=pltpu.SMEM)
VMEM = pl.BlockSpec(memory_space=pltpu.VMEM)


def call(kernel, scalars, arrays, out_shape):
    single = not isinstance(out_shape, (list, tuple))
    return pl.pallas_call(
        kernel,
        in_specs=[SMEM] * len(scalars) + [VMEM] * len(arrays),
        out_specs=VMEM if single else [VMEM] * len(out_shape),
        out_shape=out_shape,
        compiler_params=pltpu.CompilerParams(vmem_limit_bytes=48 * 1024 * 1024),
    )(*scalars, *arrays)


def group_columns(array, group):
    pieces = [
        array[:, group * GROUP_Q : (group + 1) * GROUP_Q],
        array[:, 896 + group * 64 : 960 + group * 64],
        array[:, 1024 + group * 64 : 1088 + group * 64],
    ]
    return jnp.concatenate(pieces, axis=1)


def whole_columns(zero, one):
    return jnp.concatenate(
        [
            zero[:, :448],
            one[:, :448],
            zero[:, 448:512],
            one[:, 448:512],
            zero[:, 512:576],
            one[:, 512:576],
        ],
        axis=1,
    )


def pad_lanes(array, width):
    return jnp.pad(array, ((0, 0), (0, width - array.shape[1])))


def adam_direction(gradient, moment_one, moment_two, clip_scale):
    clipped = gradient * clip_scale
    first_new = beta_one * moment_one + (1.0 - beta_one) * clipped
    second_new = beta_two * moment_two + (1.0 - beta_two) * clipped * clipped
    first_hat = first_new / (1.0 - beta_one**step_number)
    second_hat = second_new / (1.0 - beta_two**step_number)
    return first_hat / (jnp.sqrt(second_hat) + adam_eps)


def per_device(
    tokens,
    member_ids,
    norm_gain,
    weight,
    qkv_bias,
    fast_in,
    fast_out,
    cotangent,
    weight_first,
    weight_second,
    in_first,
    in_second,
    out_first,
    out_second,
):
    here = lax.axis_index(AXIS)
    core = here % 2
    x_spot = (here // (2 * NZ)) % NX
    y_spot = here // (2 * NZ * NX)
    is_zero = core == 0

    spread = call(split_kernel, [], [weight], jax.ShapeDtypeStruct((2 * NZ, 8, LANES), bf16))
    column = lax.all_to_all(
        spread, AXIS, split_axis=0, concat_axis=0, tiled=True, axis_index_groups=COLUMNS
    ).reshape(NZ * 16, LANES)
    column, tokens, cotangent, member_ids = lax.optimization_barrier(
        (column, tokens, cotangent, member_ids)
    )
    others = [shift(column, INNER_RINGS, j) for j in (1, 2, 3)]
    plane_a = jnp.concatenate([column, others[0]], axis=0)
    plane_b = jnp.concatenate(others[1:], axis=0)
    right_a = shift(plane_a, OUTER_RINGS, 1)
    left_b = shift(plane_b, OUTER_RINGS, -1)
    right_b = shift(plane_b, OUTER_RINGS, 1)
    left_a = shift(plane_a, OUTER_RINGS, -1)
    far_a = shift(right_a, OUTER_RINGS, 1)
    far_b = shift(left_b, OUTER_RINGS, -1)

    partner_tokens = shift(tokens, PAIRS, 1)
    cot_zero = pad_lanes(cotangent[:, :GROUP_Q], 512)
    cot_one = pad_lanes(cotangent[:, GROUP_Q:], 512)
    cot_own = jnp.where(is_zero, cot_zero, cot_one)
    cot_partner = shift(jnp.where(is_zero, cot_one, cot_zero), PAIRS, 1)
    member_tile = jnp.broadcast_to(member_ids.astype(f32)[:, None], (8, 128))
    partner_member = shift(member_tile, PAIRS, 1)[0, 0].astype(jnp.int32)
    members = jnp.stack([member_ids[0], partner_member])
    pick = (members[:, None] == jnp.arange(4, dtype=jnp.int32)[None, :]).astype(f32)
    rates = jnp.sum(pick[:, :, None] * fast_in[None], axis=1)
    slopes_all = jnp.sum(pick[:, :, None] * fast_out[None], axis=1)
    slopes = pad_lanes(
        jnp.where(is_zero, group_columns(slopes_all, 0), group_columns(slopes_all, 1)), LANES
    )
    bias_all = qkv_bias[None, :]
    bias = pad_lanes(jnp.where(is_zero, group_columns(bias_all, 0), group_columns(bias_all, 1)), LANES)
    gain = norm_gain[None, :]
    factors = jnp.concatenate([fast_in, jnp.ones((4, FEATURES), f32)])
    cosine, sine = rope_tables()

    turn = jnp.arange(TILES, dtype=jnp.int32)
    outer, inner = turn // 4, turn % 4
    y_back = jnp.where(is_zero, outer, inner)
    x_back = jnp.where(is_zero, inner, outer)
    tile_of = ((y_spot - y_back) % NY) * NX + (x_spot - x_back) % NX

    scaled = call(
        scale_kernel, [tile_of], [tokens, partner_tokens, gain, rates], [jax.ShapeDtypeStruct((2 * SEQ, 512), bf16)] * 4
    )
    partial = call(
        project_kernel,
        [],
        [scaled[0], scaled[1], scaled[3], plane_a, plane_b, right_a, right_b, left_a, left_b],
        jax.ShapeDtypeStruct((2 * SEQ, LANES), f32),
    )
    far_scaled = [shift(scaled[j], OUTER_RINGS, -j) for j in (1, 2, 3)]
    down = call(
        attention_kernel,
        [members],
        [scaled[2], partial, far_a, far_b, slopes, bias, cosine, sine, cot_own, cot_partner],
        jax.ShapeDtypeStruct((2 * SEQ, LANES), bf16),
    )
    down_back = shift(down, OUTER_RINGS, 1)
    down_ahead = shift(down, OUTER_RINGS, -1)
    sums = [
        jax.ShapeDtypeStruct((512, LANES), f32),
        jax.ShapeDtypeStruct((8, 512), f32),
        jax.ShapeDtypeStruct((SEQ, 128), f32),
    ]
    near = call(near_kernel, [], [scaled[0], down, plane_a, plane_b], sums)
    down_far_a = shift(down_back[:SEQ], OUTER_RINGS, 1)
    down_far_b = shift(down_ahead[SEQ:], OUTER_RINGS, -1)
    middle = call(
        middle_kernel, [], [far_scaled[0], down_ahead, far_scaled[2], down_back, plane_a, plane_b, *near], sums
    )
    parts = call(
        last_kernel,
        [tile_of],
        [far_scaled[1], down_far_a, down_far_b, plane_a, plane_b, *middle, factors],
        [jax.ShapeDtypeStruct((SEQ, LANES), f32)] + [jax.ShapeDtypeStruct((SEQ, LANES), bf16)] * 3,
    )
    got = [shift(parts[j], INNER_RINGS, -j) for j in (2, 1, 3)]
    column_sum = parts[0] + sum(g.astype(f32) for g in got)
    pieces = lax.all_to_all(
        column_sum.astype(bf16).reshape(2 * NZ, 8, LANES),
        AXIS,
        split_axis=0,
        concat_axis=0,
        tiled=True,
        axis_index_groups=COLUMNS,
    )
    grad_rows, packed = call(
        pack_kernel, [], [pieces], [jax.ShapeDtypeStruct((8, 1152), f32), jax.ShapeDtypeStruct((1, 128), f32)]
    )
    everyone = lax.all_to_all(
        jnp.broadcast_to(packed[:, None], (256, 1, 128)), AXIS, split_axis=0, concat_axis=0, tiled=True
    ).reshape(256, 128)
    return tuple(
        call(
            finish_kernel,
            [],
            [everyone, grad_rows, weight_first, weight_second, in_first, in_second, out_first, out_second],
            [
                jax.ShapeDtypeStruct((8, 1152), f32),
                jax.ShapeDtypeStruct((4, FEATURES), f32),
                jax.ShapeDtypeStruct((4, 1152), f32),
            ],
        )
    )


def solution(mesh):
    return jax.shard_map(
        per_device,
        mesh=mesh,
        in_specs=(
            P(AXIS, None),
            P(AXIS),
            P(),
            P(AXIS, None),
            P(),
            P(),
            P(),
            P(AXIS, None),
            P(AXIS, None),
            P(AXIS, None),
            P(),
            P(),
            P(),
            P(),
        ),
        out_specs=(P(AXIS, None), P(), P()),
        check_vma=False,
    )
```

```python
import math

import jax
import jax.numpy as jnp
from jax import lax
from jax.experimental import pallas as pl
from jax.experimental.pallas import tpu as pltpu
from jax.sharding import PartitionSpec as P


AXIS = "fsdp"
NY, NX, NZ = 4, 4, 8
HEAD_DIM = 64
GROUP_Q = 448
LANES = 640
SEQ = 128
FEATURES = 2048
TILES = FEATURES // 128

norm_eps = 1e-06
clip_limit = 1.0
beta_one = 0.9
beta_two = 0.95
adam_eps = 1e-08
rope_base = 1000000.0
step_number = 10.0


f32 = jnp.float32
bf16 = jnp.bfloat16


def device_of(y, x, z, c):
    return ((y * NX + x) * NZ + z) * 2 + c


COLUMNS = [
    [device_of(y, x, z, c) for z in range(NZ) for c in range(2)] for y in range(NY) for x in range(NX)
]
PAIRS = [
    [device_of(y, x, z, c) for c in range(2)] for y in range(NY) for x in range(NX) for z in range(NZ)
]
INNER_RINGS = [
    [device_of(y, x, z, 0) for x in range(NX)] for y in range(NY) for z in range(NZ)
] + [[device_of(y, x, z, 1) for y in range(NY)] for x in range(NX) for z in range(NZ)]
OUTER_RINGS = [
    [device_of(y, x, z, 0) for y in range(NY)] for x in range(NX) for z in range(NZ)
] + [[device_of(y, x, z, 1) for x in range(NX)] for y in range(NY) for z in range(NZ)]


def shift(array, rings, step):
    pairs = [(ring[i], ring[(i + step) % len(ring)]) for ring in rings for i in range(len(ring))]
    return lax.ppermute(array, AXIS, pairs)


def rope_tables():
    half_width = HEAD_DIM // 2
    spacing = jnp.arange(half_width, dtype=f32) * (2.0 / HEAD_DIM)
    frequency = jnp.exp(-math.log(rope_base) * spacing)
    angles = jnp.arange(SEQ, dtype=f32)[:, None] * frequency[None, :]
    cosine, sine = jnp.cos(angles), jnp.sin(angles)
    return (
        jnp.concatenate([cosine] * 4, axis=1),
        jnp.concatenate([-sine, sine, -sine, sine], axis=1),
    )


def dot(left, right, left_dim, right_dim):
    return lax.dot_general(
        left, right, (((left_dim,), (right_dim,)), ((), ())), preferred_element_type=f32
    )


def scale_kernel(tile_of, own, partner, gain, rates, *scaled):
    for part, tokens in enumerate((own, partner)):
        rows = slice(part * SEQ, (part + 1) * SEQ)
        wide = tokens[...].astype(f32)
        inv = lax.rsqrt(jnp.mean(wide * wide, axis=1, keepdims=True) + norm_eps)
        for i in range(TILES):
            lanes = pl.ds(pl.multiple_of(tile_of[i] * 128, 128), 128)
            normed = tokens[:, lanes].astype(f32) * inv * gain[:, lanes]
            spot = slice(i % 4 * 128, (i % 4 + 1) * 128)
            scaled[i // 4][rows, spot] = (normed * rates[part : part + 1, lanes]).astype(bf16)


def project_kernel(scaled0, scaled1, scaled3, *refs):
    halves, partial = refs[:-1], refs[-1]
    partial[...] = sum(
        dot(scaled[:, half * 256 : (half + 1) * 256], halves[2 * j + half][...], 1, 0)
        for j, scaled in enumerate((scaled0, scaled1, scaled3))
        for half in range(2)
    )


def attention_kernel(
    members, scaled2, partial, far_a, far_b, slopes, bias, cosine_ref, sine_ref, cot_own, cot_partner, down
):
    cosine = cosine_ref[...]
    sine = sine_ref[...]
    lane = lax.broadcasted_iota(jnp.int32, (SEQ, 128), 1)
    row = lax.broadcasted_iota(jnp.int32, (SEQ, 128), 0)
    low = lane < 64
    first = (lane & 63) < 32
    causal = jnp.concatenate([row >= lane] * 4, axis=0)
    score_scale = 1.0 / math.sqrt(HEAD_DIM)

    def swap(tile):
        return jnp.where(first, pltpu.roll(tile, 96, 1), pltpu.roll(tile, 32, 1))

    def half_turn(tile):
        return pltpu.roll(tile, 64, 1)

    projected = (
        partial[...]
        + dot(scaled2[:, :256], far_a[...], 1, 0)
        + dot(scaled2[:, 256:], far_b[...], 1, 0)
    )
    totals = []
    for part, cot in enumerate((cot_own, cot_partner)):
        rows = slice(part * SEQ, (part + 1) * SEQ)
        raw = projected[rows]
        slope = slopes[part : part + 1, :]
        biased = raw * slope + bias[...]
        turned = []
        for t in range(4):
            tile = biased[:, t * 128 : (t + 1) * 128]
            turned.append(tile * cosine + swap(tile) * sine)
        keys = turned[3]
        values = biased[:, 512:640]
        key_pair = jnp.concatenate(
            [jnp.where(low, half_turn(keys), 0.0), jnp.where(low, 0.0, keys)], axis=0
        ).astype(bf16)
        value_pair = jnp.concatenate(
            [jnp.where(low, values, 0.0), jnp.where(low, 0.0, half_turn(values))], axis=0
        ).astype(bf16)
        query = jnp.concatenate([q.astype(bf16) for q in turned], axis=0)
        upstream = jnp.concatenate([cot[:, t * 128 : (t + 1) * 128] for t in range(4)], axis=0)
        scores = dot(query, key_pair, 1, 1)
        grad_probs = dot(upstream, value_pair, 1, 1)
        probs_bf, grads_bf = [], []
        for h in range(2):
            side = slice(h * SEQ, (h + 1) * SEQ)
            masked = jnp.where(causal, scores[:, side] * score_scale, -jnp.inf)
            raised = jnp.exp(masked - jnp.max(masked, axis=1, keepdims=True))
            probs = raised * (1.0 / jnp.sum(raised, axis=1, keepdims=True))
            gp = grad_probs[:, side]
            centre = jnp.sum(gp * probs, axis=1, keepdims=True)
            probs_bf.append(probs.astype(bf16))
            grads_bf.append((probs * (gp - centre) * score_scale).astype(bf16))
        probs_pair = jnp.concatenate(probs_bf, axis=1)
        grad_pair = jnp.concatenate(grads_bf, axis=1)
        all_grads = dot(grad_pair, key_pair, 1, 0)
        key_sum = dot(grad_pair, query, 0, 0)
        value_sum = dot(probs_pair, upstream, 0, 0)
        grad_key = jnp.where(low, 0.0, half_turn(key_sum[:SEQ]) + key_sum[SEQ:])
        grad_value = jnp.where(low, value_sum[:SEQ] + half_turn(value_sum[SEQ:]), 0.0)
        grads = [all_grads[t * SEQ : (t + 1) * SEQ] for t in range(4)]
        grads[3] = jnp.where(low, grads[3], grad_key)
        grads = [g * cosine - swap(g) * sine for g in grads] + [grad_value]
        grad_biased = jnp.concatenate(grads, axis=1)
        totals.append(jnp.sum(raw * grad_biased, axis=0, keepdims=True))
        down[rows, :] = (grad_biased * slope).astype(bf16)
    spread = jnp.zeros((SEQ, 128), f32)
    for part in range(2):
        for t in range(5):
            spread += jnp.where(
                row == 64 + 4 * t + members[part], totals[part][:, t * 128 : (t + 1) * 128], 0.0
            )
    spread = spread.T
    high = spread.astype(bf16).astype(f32)
    spread = high + pltpu.roll(spread - high, 20, 1)
    for part in range(2):
        rows = slice(part * SEQ, (part + 1) * SEQ)
        tail = jnp.where(lane == 127, members[part].astype(f32), 0.0)
        if part == 0:
            tail = jnp.where(lane == 127, tail, spread)
        last = down[rows, 512:640].astype(f32)
        down[rows, 512:640] = jnp.where(low, last, tail).astype(bf16)


def weight_terms(scaled, down, planes, carry):
    grads, totals, tails = carry
    back = jnp.concatenate([dot(down, plane[...], 1, 1) for plane in planes], axis=1)
    grads = grads + dot(scaled, down, 0, 0)
    row = lax.broadcasted_iota(jnp.int32, (8, 512), 0)
    for part in range(scaled.shape[0] // SEQ):
        rows = slice(part * SEQ, (part + 1) * SEQ)
        member = down[part * SEQ : part * SEQ + 1, 639:640].astype(f32).astype(jnp.int32)
        total = jnp.sum(scaled[rows].astype(f32) * back[rows], axis=0, keepdims=True)
        totals = totals + jnp.where(row == member, total, 0.0)
    return grads, totals, tails


def near_kernel(scaled, down, plane_a, plane_b, grads, totals, tails):
    zero = (jnp.zeros((512, LANES), f32), jnp.zeros((8, 512), f32), None)
    total = weight_terms(scaled[...], down[...], (plane_a, plane_b), zero)
    grads[...], totals[...] = total[:2]
    tails[...] = down[:SEQ, 512:].astype(f32)


def middle_kernel(scaled, down, plane_a, plane_b, grads_in, totals_in, tails_in, grads, totals, tails):
    total = (grads_in[...], totals_in[...], None)
    total = weight_terms(scaled[...], down[...], (plane_a, plane_b), total)
    grads[...], totals[...] = total[:2]
    tails[...] = tails_in[...] + down[:SEQ, 512:].astype(f32)


def last_kernel(
    tile_of, scaled1, down1, scaled3, down3, plane_a, plane_b, grads_in, totals_in, tails_in, rates, *parts
):
    total = (grads_in[...], totals_in[...], None)
    total = weight_terms(scaled1[...], down1[...], (plane_a, plane_b), total)
    grads, totals, _ = weight_terms(scaled3[...], down3[...], (plane_a, plane_b), total)
    tails = tails_in[...] + down1[:SEQ, 512:].astype(f32) + down3[:SEQ, 512:].astype(f32)
    tails = tails + pltpu.roll(tails, 108, 1)
    lane = lax.broadcasted_iota(jnp.int32, (SEQ, 128), 1)
    for i, result in enumerate(parts):
        tile = tile_of[i]
        here = slice(i * 128, (i + 1) * 128)
        shares = totals[:, here] / rates[:, pl.ds(pl.multiple_of(tile * 128, 128), 128)]
        extra = jnp.concatenate([jnp.zeros((64, 128), f32), shares, jnp.zeros((56, 128), f32)], axis=0).T
        for t in range(5):
            moved = pltpu.roll(tails, (4 - 4 * t) % 128, 1)
            extra = jnp.where((lane >= 68) & (lane < 72) & (tile == t), moved, extra)
        result[:, :512] = grads[here, :512].astype(result.dtype)
        result[:, 512:] = jnp.where(lane < 64, grads[here, 512:], extra).astype(result.dtype)


def split_kernel(weight, spread):
    rows = weight[...]
    for core in range(2):
        cols = pad_lanes(group_columns(rows, core), LANES)
        for z in range(NZ):
            spread[2 * z + core, :, :] = cols


def exact_dot(values, picks):
    high = values.astype(bf16)
    rest = values - high.astype(f32)
    middle = rest.astype(bf16)
    low = (rest - middle.astype(f32)).astype(bf16)
    return dot(high, picks, 1, 0) + dot(middle, picks, 1, 0) + dot(low, picks, 1, 0)


def pack_kernel(pieces, grad_rows, packed):
    wide = pieces[...].astype(f32)
    sums = [sum(wide[2 * z + core] for z in range(NZ)) for core in range(2)]
    grads = whole_columns(*sums)
    grad_rows[...] = grads
    square = jnp.sum(jnp.sum(grads * grads, axis=1, keepdims=True), axis=0, keepdims=True)
    tails = [s[:, 512:] for s in sums]
    source = lax.broadcasted_iota(jnp.int32, (128, 128), 0)
    target = lax.broadcasted_iota(jnp.int32, (128, 128), 1)
    field = target // 8
    from_in = ((source == 64 + field) & (field < 4)).astype(bf16)
    from_zero = ((source == 64 + field) & (field >= 4) & (field < 8)).astype(bf16)
    from_one = ((source == 60 + field) & (field >= 8) & (field < 12)).astype(bf16)
    moved = (
        exact_dot(tails[0] + tails[1], from_in)
        + exact_dot(tails[0], from_zero)
        + exact_dot(tails[1], from_one)
    )
    row = lax.broadcasted_iota(jnp.int32, (8, 128), 0)
    lane = lax.broadcasted_iota(jnp.int32, (8, 128), 1)
    line = jnp.sum(jnp.where(row == (lane & 7), moved, 0.0), axis=0, keepdims=True)
    packed[...] = jnp.where(lane[:1] == 96, square, line)


def finish_kernel(
    everyone, grad_rows, weight_first, weight_second, in_first, in_second, out_first, out_second,
    weight_step, in_step, out_step,
):
    shares = everyone[...]
    lane = lax.broadcasted_iota(jnp.int32, (256, 128), 1)
    row = lax.broadcasted_iota(jnp.int32, (256, 128), 0)
    source = lax.broadcasted_iota(jnp.int32, (128, 128), 0)
    target = lax.broadcasted_iota(jnp.int32, (128, 128), 1)
    mine = (row & 15) == lane // 8
    fields = []
    for field in range(12):
        picks = (source == 8 * field + (target & 7)).astype(bf16)
        moved = jnp.where(mine, exact_dot(shares, picks), 0.0)
        fields.append(jnp.sum(moved.reshape(16, 16, 128), axis=1))

    def as_rows(start, tiles):
        return jnp.concatenate(
            [jnp.concatenate([f[t : t + 1] for t in range(tiles)], axis=1) for f in fields[start : start + 4]],
            axis=0,
        )

    in_grad = as_rows(0, TILES)
    out_grad = whole_columns(as_rows(4, 5), as_rows(8, 5))

    def total(values):
        return jnp.sum(jnp.sum(values, axis=1, keepdims=True), axis=0, keepdims=True)

    squared = (
        total(jnp.where(lane == 96, shares, 0.0)) + total(in_grad * in_grad) + total(out_grad * out_grad)
    )
    clip_scale = clip_limit / jnp.maximum(jnp.sqrt(squared), clip_limit)
    weight_step[...] = adam_direction(grad_rows[...], weight_first[...], weight_second[...], clip_scale)
    in_step[...] = adam_direction(in_grad, in_first[...], in_second[...], clip_scale)
    out_step[...] = adam_direction(out_grad, out_first[...], out_second[...], clip_scale)


SMEM = pl.BlockSpec(memory_space=pltpu.SMEM)
VMEM = pl.BlockSpec(memory_space=pltpu.VMEM)


def call(kernel, scalars, arrays, out_shape):
    single = not isinstance(out_shape, (list, tuple))
    return pl.pallas_call(
        kernel,
        in_specs=[SMEM] * len(scalars) + [VMEM] * len(arrays),
        out_specs=VMEM if single else [VMEM] * len(out_shape),
        out_shape=out_shape,
        compiler_params=pltpu.CompilerParams(vmem_limit_bytes=48 * 1024 * 1024),
    )(*scalars, *arrays)


def group_columns(array, group):
    pieces = [
        array[:, group * GROUP_Q : (group + 1) * GROUP_Q],
        array[:, 896 + group * 64 : 960 + group * 64],
        array[:, 1024 + group * 64 : 1088 + group * 64],
    ]
    return jnp.concatenate(pieces, axis=1)


def whole_columns(zero, one):
    return jnp.concatenate(
        [
            zero[:, :448],
            one[:, :448],
            zero[:, 448:512],
            one[:, 448:512],
            zero[:, 512:576],
            one[:, 512:576],
        ],
        axis=1,
    )


def pad_lanes(array, width):
    return jnp.pad(array, ((0, 0), (0, width - array.shape[1])))


def adam_direction(gradient, moment_one, moment_two, clip_scale):
    clipped = gradient * clip_scale
    first_new = beta_one * moment_one + (1.0 - beta_one) * clipped
    second_new = beta_two * moment_two + (1.0 - beta_two) * clipped * clipped
    first_hat = first_new / (1.0 - beta_one**step_number)
    second_hat = second_new / (1.0 - beta_two**step_number)
    return first_hat / (jnp.sqrt(second_hat) + adam_eps)


def per_device(
    tokens,
    member_ids,
    norm_gain,
    weight,
    qkv_bias,
    fast_in,
    fast_out,
    cotangent,
    weight_first,
    weight_second,
    in_first,
    in_second,
    out_first,
    out_second,
):
    here = lax.axis_index(AXIS)
    core = here % 2
    x_spot = (here // (2 * NZ)) % NX
    y_spot = here // (2 * NZ * NX)
    is_zero = core == 0

    spread = call(split_kernel, [], [weight], jax.ShapeDtypeStruct((2 * NZ, 8, LANES), bf16))
    column = lax.all_to_all(
        spread, AXIS, split_axis=0, concat_axis=0, tiled=True, axis_index_groups=COLUMNS
    ).reshape(NZ * 16, LANES)
    column, cotangent = lax.optimization_barrier((column, cotangent))
    others = [shift(column, INNER_RINGS, j) for j in (1, 2, 3)]
    plane_a = jnp.concatenate([column, others[0]], axis=0)
    plane_b = jnp.concatenate(others[1:], axis=0)
    right_a = shift(plane_a, OUTER_RINGS, 1)
    left_b = shift(plane_b, OUTER_RINGS, -1)
    right_b = shift(plane_b, OUTER_RINGS, 1)
    left_a = shift(plane_a, OUTER_RINGS, -1)
    far_a = shift(right_a, OUTER_RINGS, 1)
    far_b = shift(left_b, OUTER_RINGS, -1)

    partner_tokens = shift(tokens, PAIRS, 1)
    cot_zero = pad_lanes(cotangent[:, :GROUP_Q], 512)
    cot_one = pad_lanes(cotangent[:, GROUP_Q:], 512)
    cot_own = jnp.where(is_zero, cot_zero, cot_one)
    cot_partner = shift(jnp.where(is_zero, cot_one, cot_zero), PAIRS, 1)
    member_tile = jnp.broadcast_to(member_ids.astype(f32)[:, None], (8, 128))
    partner_member = shift(member_tile, PAIRS, 1)[0, 0].astype(jnp.int32)
    members = jnp.stack([member_ids[0], partner_member])
    pick = (members[:, None] == jnp.arange(4, dtype=jnp.int32)[None, :]).astype(f32)
    rates = jnp.sum(pick[:, :, None] * fast_in[None], axis=1)
    slopes_all = jnp.sum(pick[:, :, None] * fast_out[None], axis=1)
    slopes = pad_lanes(
        jnp.where(is_zero, group_columns(slopes_all, 0), group_columns(slopes_all, 1)), LANES
    )
    bias_all = qkv_bias[None, :]
    bias = pad_lanes(jnp.where(is_zero, group_columns(bias_all, 0), group_columns(bias_all, 1)), LANES)
    gain = norm_gain[None, :]
    factors = jnp.concatenate([fast_in, jnp.ones((4, FEATURES), f32)])
    cosine, sine = rope_tables()

    turn = jnp.arange(TILES, dtype=jnp.int32)
    outer, inner = turn // 4, turn % 4
    y_back = jnp.where(is_zero, outer, inner)
    x_back = jnp.where(is_zero, inner, outer)
    tile_of = ((y_spot - y_back) % NY) * NX + (x_spot - x_back) % NX

    scaled = call(
        scale_kernel, [tile_of], [tokens, partner_tokens, gain, rates], [jax.ShapeDtypeStruct((2 * SEQ, 512), bf16)] * 4
    )
    partial = call(
        project_kernel,
        [],
        [scaled[0], scaled[1], scaled[3], plane_a, plane_b, right_a, right_b, left_a, left_b],
        jax.ShapeDtypeStruct((2 * SEQ, LANES), f32),
    )
    far_scaled = [shift(scaled[j], OUTER_RINGS, -j) for j in (1, 2, 3)]
    down = call(
        attention_kernel,
        [members],
        [scaled[2], partial, far_a, far_b, slopes, bias, cosine, sine, cot_own, cot_partner],
        jax.ShapeDtypeStruct((2 * SEQ, LANES), bf16),
    )
    down_of = [shift(down, OUTER_RINGS, -j) for j in (1, 2, 3)]
    sums = [
        jax.ShapeDtypeStruct((512, LANES), f32),
        jax.ShapeDtypeStruct((8, 512), f32),
        jax.ShapeDtypeStruct((SEQ, 128), f32),
    ]
    near = call(near_kernel, [], [scaled[0], down, plane_a, plane_b], sums)
    middle = call(middle_kernel, [], [far_scaled[1], down_of[1], plane_a, plane_b, *near], sums)
    parts = call(
        last_kernel,
        [tile_of],
        [far_scaled[0], down_of[0], far_scaled[2], down_of[2], plane_a, plane_b, *middle, factors],
        [jax.ShapeDtypeStruct((SEQ, LANES), f32)] + [jax.ShapeDtypeStruct((SEQ, LANES), bf16)] * 3,
    )
    got = [shift(parts[j], INNER_RINGS, -j) for j in (1, 2, 3)]
    column_sum = parts[0] + sum(g.astype(f32) for g in got)
    pieces = lax.all_to_all(
        column_sum.astype(bf16).reshape(2 * NZ, 8, LANES),
        AXIS,
        split_axis=0,
        concat_axis=0,
        tiled=True,
        axis_index_groups=COLUMNS,
    )
    grad_rows, packed = call(
        pack_kernel, [], [pieces], [jax.ShapeDtypeStruct((8, 1152), f32), jax.ShapeDtypeStruct((1, 128), f32)]
    )
    everyone = lax.all_to_all(
        jnp.broadcast_to(packed[:, None], (256, 1, 128)), AXIS, split_axis=0, concat_axis=0, tiled=True
    ).reshape(256, 128)
    return tuple(
        call(
            finish_kernel,
            [],
            [everyone, grad_rows, weight_first, weight_second, in_first, in_second, out_first, out_second],
            [
                jax.ShapeDtypeStruct((8, 1152), f32),
                jax.ShapeDtypeStruct((4, FEATURES), f32),
                jax.ShapeDtypeStruct((4, 1152), f32),
            ],
        )
    )


def solution(mesh):
    return jax.shard_map(
        per_device,
        mesh=mesh,
        in_specs=(
            P(AXIS, None),
            P(AXIS),
            P(),
            P(AXIS, None),
            P(),
            P(),
            P(),
            P(AXIS, None),
            P(AXIS, None),
            P(AXIS, None),
            P(),
            P(),
            P(),
            P(),
        ),
        out_specs=(P(AXIS, None), P(), P()),
        check_vma=False,
    )
```

```python
import math

import jax
import jax.numpy as jnp
from jax import lax
from jax.experimental import pallas as pl
from jax.experimental.pallas import tpu as pltpu
from jax.sharding import PartitionSpec as P


AXIS = "fsdp"
NY, NX, NZ = 4, 4, 8
HEAD_DIM = 64
GROUP_Q = 448
LANES = 640
SEQ = 128
FEATURES = 2048
TILES = FEATURES // 128

norm_eps = 1e-06
clip_limit = 1.0
beta_one = 0.9
beta_two = 0.95
adam_eps = 1e-08
rope_base = 1000000.0
step_number = 10.0


f32 = jnp.float32
bf16 = jnp.bfloat16


def device_of(y, x, z, c):
    return ((y * NX + x) * NZ + z) * 2 + c


COLUMNS = [
    [device_of(y, x, z, c) for z in range(NZ) for c in range(2)] for y in range(NY) for x in range(NX)
]
PAIRS = [
    [device_of(y, x, z, c) for c in range(2)] for y in range(NY) for x in range(NX) for z in range(NZ)
]
INNER_RINGS = [
    [device_of(y, x, z, 0) for x in range(NX)] for y in range(NY) for z in range(NZ)
] + [[device_of(y, x, z, 1) for y in range(NY)] for x in range(NX) for z in range(NZ)]
OUTER_RINGS = [
    [device_of(y, x, z, 0) for y in range(NY)] for x in range(NX) for z in range(NZ)
] + [[device_of(y, x, z, 1) for x in range(NX)] for y in range(NY) for z in range(NZ)]


def shift(array, rings, step):
    pairs = [(ring[i], ring[(i + step) % len(ring)]) for ring in rings for i in range(len(ring))]
    return lax.ppermute(array, AXIS, pairs)


def rope_tables():
    half_width = HEAD_DIM // 2
    spacing = jnp.arange(half_width, dtype=f32) * (2.0 / HEAD_DIM)
    frequency = jnp.exp(-math.log(rope_base) * spacing)
    angles = jnp.arange(SEQ, dtype=f32)[:, None] * frequency[None, :]
    cosine, sine = jnp.cos(angles), jnp.sin(angles)
    return (
        jnp.concatenate([cosine] * 4, axis=1),
        jnp.concatenate([-sine, sine, -sine, sine], axis=1),
    )


def dot(left, right, left_dim, right_dim):
    return lax.dot_general(
        left, right, (((left_dim,), (right_dim,)), ((), ())), preferred_element_type=f32
    )


def scale_kernel(tile_of, own, partner, gain, rates, *scaled):
    for part, tokens in enumerate((own, partner)):
        rows = slice(part * SEQ, (part + 1) * SEQ)
        wide = tokens[...].astype(f32)
        inv = lax.rsqrt(jnp.mean(wide * wide, axis=1, keepdims=True) + norm_eps)
        for i in range(TILES):
            lanes = pl.ds(pl.multiple_of(tile_of[i] * 128, 128), 128)
            normed = tokens[:, lanes].astype(f32) * inv * gain[:, lanes]
            spot = slice(i % 4 * 128, (i % 4 + 1) * 128)
            scaled[i // 4][rows, spot] = (normed * rates[part : part + 1, lanes]).astype(bf16)


def project_kernel(scaled0, scaled1, scaled3, *refs):
    halves, partial = refs[:-1], refs[-1]
    partial[...] = sum(
        dot(scaled[:, half * 256 : (half + 1) * 256], halves[2 * j + half][...], 1, 0)
        for j, scaled in enumerate((scaled0, scaled1, scaled3))
        for half in range(2)
    )


def attention_kernel(
    members, scaled2, partial, far_a, far_b, slopes, bias, cosine_ref, sine_ref, cot_own, cot_partner, down
):
    cosine = cosine_ref[...]
    sine = sine_ref[...]
    lane = lax.broadcasted_iota(jnp.int32, (SEQ, 128), 1)
    row = lax.broadcasted_iota(jnp.int32, (SEQ, 128), 0)
    low = lane < 64
    first = (lane & 63) < 32
    causal = jnp.concatenate([row >= lane] * 4, axis=0)
    score_scale = 1.0 / math.sqrt(HEAD_DIM)

    def swap(tile):
        return jnp.where(first, pltpu.roll(tile, 96, 1), pltpu.roll(tile, 32, 1))

    def half_turn(tile):
        return pltpu.roll(tile, 64, 1)

    projected = (
        partial[...]
        + dot(scaled2[:, :256], far_a[...], 1, 0)
        + dot(scaled2[:, 256:], far_b[...], 1, 0)
    )
    totals = []
    for part, cot in enumerate((cot_own, cot_partner)):
        rows = slice(part * SEQ, (part + 1) * SEQ)
        raw = projected[rows]
        slope = slopes[part : part + 1, :]
        biased = raw * slope + bias[...]
        turned = []
        for t in range(4):
            tile = biased[:, t * 128 : (t + 1) * 128]
            turned.append(tile * cosine + swap(tile) * sine)
        keys = turned[3]
        values = biased[:, 512:640]
        key_pair = jnp.concatenate(
            [jnp.where(low, half_turn(keys), 0.0), jnp.where(low, 0.0, keys)], axis=0
        ).astype(bf16)
        value_pair = jnp.concatenate(
            [jnp.where(low, values, 0.0), jnp.where(low, 0.0, half_turn(values))], axis=0
        ).astype(bf16)
        query = jnp.concatenate([q.astype(bf16) for q in turned], axis=0)
        upstream = jnp.concatenate([cot[:, t * 128 : (t + 1) * 128] for t in range(4)], axis=0)
        scores = dot(query, key_pair, 1, 1)
        grad_probs = dot(upstream, value_pair, 1, 1)
        probs_bf, grads_bf = [], []
        for h in range(2):
            side = slice(h * SEQ, (h + 1) * SEQ)
            masked = jnp.where(causal, scores[:, side] * score_scale, -jnp.inf)
            raised = jnp.exp(masked - jnp.max(masked, axis=1, keepdims=True))
            probs = raised * (1.0 / jnp.sum(raised, axis=1, keepdims=True))
            gp = grad_probs[:, side]
            centre = jnp.sum(gp * probs, axis=1, keepdims=True)
            probs_bf.append(probs.astype(bf16))
            grads_bf.append((probs * (gp - centre) * score_scale).astype(bf16))
        probs_pair = jnp.concatenate(probs_bf, axis=1)
        grad_pair = jnp.concatenate(grads_bf, axis=1)
        all_grads = dot(grad_pair, key_pair, 1, 0)
        key_sum = dot(grad_pair, query, 0, 0)
        value_sum = dot(probs_pair, upstream, 0, 0)
        grad_key = jnp.where(low, 0.0, half_turn(key_sum[:SEQ]) + key_sum[SEQ:])
        grad_value = jnp.where(low, value_sum[:SEQ] + half_turn(value_sum[SEQ:]), 0.0)
        grads = [all_grads[t * SEQ : (t + 1) * SEQ] for t in range(4)]
        grads[3] = jnp.where(low, grads[3], grad_key)
        grads = [g * cosine - swap(g) * sine for g in grads] + [grad_value]
        grad_biased = jnp.concatenate(grads, axis=1)
        totals.append(jnp.sum(raw * grad_biased, axis=0, keepdims=True))
        down[rows, :] = (grad_biased * slope).astype(bf16)
    spread = jnp.zeros((SEQ, 128), f32)
    for part in range(2):
        for t in range(5):
            spread += jnp.where(
                row == 64 + 4 * t + members[part], totals[part][:, t * 128 : (t + 1) * 128], 0.0
            )
    spread = spread.T
    high = spread.astype(bf16).astype(f32)
    spread = high + pltpu.roll(spread - high, 20, 1)
    for part in range(2):
        rows = slice(part * SEQ, (part + 1) * SEQ)
        tail = jnp.where(lane == 127, members[part].astype(f32), 0.0)
        if part == 0:
            tail = jnp.where(lane == 127, tail, spread)
        last = down[rows, 512:640].astype(f32)
        down[rows, 512:640] = jnp.where(low, last, tail).astype(bf16)


def weight_terms(scaled, down, planes, carry):
    grads, totals, tails = carry
    back = jnp.concatenate([dot(down, plane[...], 1, 1) for plane in planes], axis=1)
    grads = grads + dot(scaled, down, 0, 0)
    row = lax.broadcasted_iota(jnp.int32, (8, 512), 0)
    for part in range(scaled.shape[0] // SEQ):
        rows = slice(part * SEQ, (part + 1) * SEQ)
        member = down[part * SEQ : part * SEQ + 1, 639:640].astype(f32).astype(jnp.int32)
        total = jnp.sum(scaled[rows].astype(f32) * back[rows], axis=0, keepdims=True)
        totals = totals + jnp.where(row == member, total, 0.0)
    return grads, totals, tails


def near_kernel(scaled, down, plane_a, plane_b, grads, totals, tails):
    zero = (jnp.zeros((512, LANES), f32), jnp.zeros((8, 512), f32), None)
    total = weight_terms(scaled[...], down[...], (plane_a, plane_b), zero)
    grads[...], totals[...] = total[:2]
    tails[...] = down[:SEQ, 512:].astype(f32)


def middle_kernel(scaled, down, plane_a, plane_b, grads_in, totals_in, tails_in, grads, totals, tails):
    total = (grads_in[...], totals_in[...], None)
    total = weight_terms(scaled[...], down[...], (plane_a, plane_b), total)
    grads[...], totals[...] = total[:2]
    tails[...] = tails_in[...] + down[:SEQ, 512:].astype(f32)


def last_kernel(
    tile_of, scaled, down, plane_a, plane_b, grads_in, totals_in, tails_in, rates, *parts
):
    total = (grads_in[...], totals_in[...], None)
    grads, totals, _ = weight_terms(scaled[...], down[...], (plane_a, plane_b), total)
    tails = tails_in[...] + down[:SEQ, 512:].astype(f32)
    tails = tails + pltpu.roll(tails, 108, 1)
    lane = lax.broadcasted_iota(jnp.int32, (SEQ, 128), 1)
    for i, result in enumerate(parts):
        tile = tile_of[i]
        here = slice(i * 128, (i + 1) * 128)
        shares = totals[:, here] / rates[:, pl.ds(pl.multiple_of(tile * 128, 128), 128)]
        extra = jnp.concatenate([jnp.zeros((64, 128), f32), shares, jnp.zeros((56, 128), f32)], axis=0).T
        for t in range(5):
            moved = pltpu.roll(tails, (4 - 4 * t) % 128, 1)
            extra = jnp.where((lane >= 68) & (lane < 72) & (tile == t), moved, extra)
        result[:, :512] = grads[here, :512].astype(result.dtype)
        result[:, 512:] = jnp.where(lane < 64, grads[here, 512:], extra).astype(result.dtype)


def split_kernel(weight, spread):
    rows = weight[...]
    for core in range(2):
        cols = pad_lanes(group_columns(rows, core), LANES)
        for z in range(NZ):
            spread[2 * z + core, :, :] = cols


def exact_dot(values, picks):
    high = values.astype(bf16)
    rest = values - high.astype(f32)
    middle = rest.astype(bf16)
    low = (rest - middle.astype(f32)).astype(bf16)
    return dot(high, picks, 1, 0) + dot(middle, picks, 1, 0) + dot(low, picks, 1, 0)


def pack_kernel(pieces, grad_rows, packed):
    wide = pieces[...].astype(f32)
    sums = [sum(wide[2 * z + core] for z in range(NZ)) for core in range(2)]
    grads = whole_columns(*sums)
    grad_rows[...] = grads
    square = jnp.sum(jnp.sum(grads * grads, axis=1, keepdims=True), axis=0, keepdims=True)
    tails = [s[:, 512:] for s in sums]
    source = lax.broadcasted_iota(jnp.int32, (128, 128), 0)
    target = lax.broadcasted_iota(jnp.int32, (128, 128), 1)
    field = target // 8
    from_in = ((source == 64 + field) & (field < 4)).astype(bf16)
    from_zero = ((source == 64 + field) & (field >= 4) & (field < 8)).astype(bf16)
    from_one = ((source == 60 + field) & (field >= 8) & (field < 12)).astype(bf16)
    moved = (
        exact_dot(tails[0] + tails[1], from_in)
        + exact_dot(tails[0], from_zero)
        + exact_dot(tails[1], from_one)
    )
    row = lax.broadcasted_iota(jnp.int32, (8, 128), 0)
    lane = lax.broadcasted_iota(jnp.int32, (8, 128), 1)
    line = jnp.sum(jnp.where(row == (lane & 7), moved, 0.0), axis=0, keepdims=True)
    packed[...] = jnp.where(lane[:1] == 96, square, line)


def finish_kernel(
    everyone, grad_rows, weight_first, weight_second, in_first, in_second, out_first, out_second,
    weight_step, in_step, out_step,
):
    shares = everyone[...]
    lane = lax.broadcasted_iota(jnp.int32, (256, 128), 1)
    row = lax.broadcasted_iota(jnp.int32, (256, 128), 0)
    source = lax.broadcasted_iota(jnp.int32, (128, 128), 0)
    target = lax.broadcasted_iota(jnp.int32, (128, 128), 1)
    mine = (row & 15) == lane // 8
    fields = []
    for field in range(12):
        picks = (source == 8 * field + (target & 7)).astype(bf16)
        moved = jnp.where(mine, exact_dot(shares, picks), 0.0)
        fields.append(jnp.sum(moved.reshape(16, 16, 128), axis=1))

    def as_rows(start, tiles):
        return jnp.concatenate(
            [jnp.concatenate([f[t : t + 1] for t in range(tiles)], axis=1) for f in fields[start : start + 4]],
            axis=0,
        )

    in_grad = as_rows(0, TILES)
    out_grad = whole_columns(as_rows(4, 5), as_rows(8, 5))

    def total(values):
        return jnp.sum(jnp.sum(values, axis=1, keepdims=True), axis=0, keepdims=True)

    squared = (
        total(jnp.where(lane == 96, shares, 0.0)) + total(in_grad * in_grad) + total(out_grad * out_grad)
    )
    clip_scale = clip_limit / jnp.maximum(jnp.sqrt(squared), clip_limit)
    weight_step[...] = adam_direction(grad_rows[...], weight_first[...], weight_second[...], clip_scale)
    in_step[...] = adam_direction(in_grad, in_first[...], in_second[...], clip_scale)
    out_step[...] = adam_direction(out_grad, out_first[...], out_second[...], clip_scale)


SMEM = pl.BlockSpec(memory_space=pltpu.SMEM)
VMEM = pl.BlockSpec(memory_space=pltpu.VMEM)


def call(kernel, scalars, arrays, out_shape):
    single = not isinstance(out_shape, (list, tuple))
    return pl.pallas_call(
        kernel,
        in_specs=[SMEM] * len(scalars) + [VMEM] * len(arrays),
        out_specs=VMEM if single else [VMEM] * len(out_shape),
        out_shape=out_shape,
        compiler_params=pltpu.CompilerParams(vmem_limit_bytes=48 * 1024 * 1024),
    )(*scalars, *arrays)


def group_columns(array, group):
    pieces = [
        array[:, group * GROUP_Q : (group + 1) * GROUP_Q],
        array[:, 896 + group * 64 : 960 + group * 64],
        array[:, 1024 + group * 64 : 1088 + group * 64],
    ]
    return jnp.concatenate(pieces, axis=1)


def whole_columns(zero, one):
    return jnp.concatenate(
        [
            zero[:, :448],
            one[:, :448],
            zero[:, 448:512],
            one[:, 448:512],
            zero[:, 512:576],
            one[:, 512:576],
        ],
        axis=1,
    )


def pad_lanes(array, width):
    return jnp.pad(array, ((0, 0), (0, width - array.shape[1])))


def adam_direction(gradient, moment_one, moment_two, clip_scale):
    clipped = gradient * clip_scale
    first_new = beta_one * moment_one + (1.0 - beta_one) * clipped
    second_new = beta_two * moment_two + (1.0 - beta_two) * clipped * clipped
    first_hat = first_new / (1.0 - beta_one**step_number)
    second_hat = second_new / (1.0 - beta_two**step_number)
    return first_hat / (jnp.sqrt(second_hat) + adam_eps)


def per_device(
    tokens,
    member_ids,
    norm_gain,
    weight,
    qkv_bias,
    fast_in,
    fast_out,
    cotangent,
    weight_first,
    weight_second,
    in_first,
    in_second,
    out_first,
    out_second,
):
    here = lax.axis_index(AXIS)
    core = here % 2
    x_spot = (here // (2 * NZ)) % NX
    y_spot = here // (2 * NZ * NX)
    is_zero = core == 0

    spread = call(split_kernel, [], [weight], jax.ShapeDtypeStruct((2 * NZ, 8, LANES), bf16))
    column = lax.all_to_all(
        spread, AXIS, split_axis=0, concat_axis=0, tiled=True, axis_index_groups=COLUMNS
    ).reshape(NZ * 16, LANES)
    column, tokens, cotangent, member_ids = lax.optimization_barrier(
        (column, tokens, cotangent, member_ids)
    )
    others = [shift(column, INNER_RINGS, j) for j in (1, 2, 3)]
    plane_a = jnp.concatenate([column, others[0]], axis=0)
    plane_b = jnp.concatenate(others[1:], axis=0)
    right_a = shift(plane_a, OUTER_RINGS, 1)
    left_b = shift(plane_b, OUTER_RINGS, -1)
    right_b = shift(plane_b, OUTER_RINGS, 1)
    left_a = shift(plane_a, OUTER_RINGS, -1)
    far_a = shift(right_a, OUTER_RINGS, 1)
    far_b = shift(left_b, OUTER_RINGS, -1)

    partner_tokens = shift(tokens, PAIRS, 1)
    cot_zero = pad_lanes(cotangent[:, :GROUP_Q], 512)
    cot_one = pad_lanes(cotangent[:, GROUP_Q:], 512)
    cot_own = jnp.where(is_zero, cot_zero, cot_one)
    cot_partner = shift(jnp.where(is_zero, cot_one, cot_zero), PAIRS, 1)
    member_tile = jnp.broadcast_to(member_ids.astype(f32)[:, None], (8, 128))
    partner_member = shift(member_tile, PAIRS, 1)[0, 0].astype(jnp.int32)
    members = jnp.stack([member_ids[0], partner_member])
    pick = (members[:, None] == jnp.arange(4, dtype=jnp.int32)[None, :]).astype(f32)
    rates = jnp.sum(pick[:, :, None] * fast_in[None], axis=1)
    slopes_all = jnp.sum(pick[:, :, None] * fast_out[None], axis=1)
    slopes = pad_lanes(
        jnp.where(is_zero, group_columns(slopes_all, 0), group_columns(slopes_all, 1)), LANES
    )
    bias_all = qkv_bias[None, :]
    bias = pad_lanes(jnp.where(is_zero, group_columns(bias_all, 0), group_columns(bias_all, 1)), LANES)
    gain = norm_gain[None, :]
    factors = jnp.concatenate([fast_in, jnp.ones((4, FEATURES), f32)])
    cosine, sine = rope_tables()

    turn = jnp.arange(TILES, dtype=jnp.int32)
    outer, inner = turn // 4, turn % 4
    y_back = jnp.where(is_zero, outer, inner)
    x_back = jnp.where(is_zero, inner, outer)
    tile_of = ((y_spot - y_back) % NY) * NX + (x_spot - x_back) % NX

    scaled = call(
        scale_kernel, [tile_of], [tokens, partner_tokens, gain, rates], [jax.ShapeDtypeStruct((2 * SEQ, 512), bf16)] * 4
    )
    partial = call(
        project_kernel,
        [],
        [scaled[0], scaled[1], scaled[3], plane_a, plane_b, right_a, right_b, left_a, left_b],
        jax.ShapeDtypeStruct((2 * SEQ, LANES), f32),
    )
    far_scaled = [shift(scaled[j], OUTER_RINGS, -j) for j in (1, 2, 3)]
    down = call(
        attention_kernel,
        [members],
        [scaled[2], partial, far_a, far_b, slopes, bias, cosine, sine, cot_own, cot_partner],
        jax.ShapeDtypeStruct((2 * SEQ, LANES), bf16),
    )
    down_of = [shift(down, OUTER_RINGS, -j) for j in (1, 2, 3)]
    sums = [
        jax.ShapeDtypeStruct((512, LANES), f32),
        jax.ShapeDtypeStruct((8, 512), f32),
        jax.ShapeDtypeStruct((SEQ, 128), f32),
    ]
    near = call(near_kernel, [], [scaled[0], down, plane_a, plane_b], sums)
    middle = near
    for j in (2, 3):
        middle = call(middle_kernel, [], [far_scaled[j - 1], down_of[j - 1], plane_a, plane_b, *middle], sums)
    parts = call(
        last_kernel,
        [tile_of],
        [far_scaled[0], down_of[0], plane_a, plane_b, *middle, factors],
        [jax.ShapeDtypeStruct((SEQ, LANES), f32)] + [jax.ShapeDtypeStruct((SEQ, LANES), bf16)] * 3,
    )
    got = [shift(parts[j], INNER_RINGS, -j) for j in (1, 2, 3)]
    column_sum = parts[0] + sum(g.astype(f32) for g in got)
    pieces = lax.all_to_all(
        column_sum.astype(bf16).reshape(2 * NZ, 8, LANES),
        AXIS,
        split_axis=0,
        concat_axis=0,
        tiled=True,
        axis_index_groups=COLUMNS,
    )
    grad_rows, packed = call(
        pack_kernel, [], [pieces], [jax.ShapeDtypeStruct((8, 1152), f32), jax.ShapeDtypeStruct((1, 128), f32)]
    )
    everyone = lax.all_to_all(
        jnp.broadcast_to(packed[:, None], (256, 1, 128)), AXIS, split_axis=0, concat_axis=0, tiled=True
    ).reshape(256, 128)
    return tuple(
        call(
            finish_kernel,
            [],
            [everyone, grad_rows, weight_first, weight_second, in_first, in_second, out_first, out_second],
            [
                jax.ShapeDtypeStruct((8, 1152), f32),
                jax.ShapeDtypeStruct((4, FEATURES), f32),
                jax.ShapeDtypeStruct((4, 1152), f32),
            ],
        )
    )


def solution(mesh):
    return jax.shard_map(
        per_device,
        mesh=mesh,
        in_specs=(
            P(AXIS, None),
            P(AXIS),
            P(),
            P(AXIS, None),
            P(),
            P(),
            P(),
            P(AXIS, None),
            P(AXIS, None),
            P(AXIS, None),
            P(),
            P(),
            P(),
            P(),
        ),
        out_specs=(P(AXIS, None), P(), P()),
        check_vma=False,
    )
```
